256 devices in a mesh: replica: 16 (over x_lo, z), expert: 16 (over x_hi, y, core).
Axes of the slice: x: 4 (x_hi: 2, x_lo: 2; x = x_hi * 2 + x_lo), y: 4, z: 8, core: 2. Of those that a mesh axis runs over, the one named last changes fastest.
Arguments:
- weights: bfloat16 [16, 2048, 512], P('expert'), may hold values from -3 to 3
- momentum: float32 [16, 16, 2048, 512], P('replica', 'expert'), may hold values from -6 to 6
- gradients: bfloat16 [2, 16, 16, 2048, 512], P(None, 'replica', 'expert'), may hold values from -6 to 6
- outer_momentum: float32 [16, 2048, 512], P('expert', 'replica'), may hold values from -2 to 2
Outputs:
- new_weights: bfloat16 [16, 2048, 512], P('expert')
- new_outer: float32 [16, 2048, 512], P('expert', 'replica')
The draws below stay inside these ranges and needn't reach their ends.
All inputs are finite; a program needn't handle non-finite values.
Results may differ from the reference program's by a relative error of at most 0.0075.
Values may be sent and summed in bfloat16 or wider, within the bound.
A program may use at most 64 MiB of HBM per device.

```python
import math
import jax
import jax.numpy as jnp
import numpy as np
from jax import lax

ROWS = 2048
COLS = 512
STEPS = 2
NS_ITERS = 3
EXPERTS = 16
REPLICAS = 16


def block_scale(rng, extent, pieces, low, largest):
    level, own = 1.0, jax.random.fold_in(rng, 6)
    for dim, shards_of in pieces:
        draws = jnp.exp(jax.random.uniform(jax.random.fold_in(own, dim), (shards_of,), jnp.float32, low / len(pieces), largest / len(pieces)))
        level = level * jnp.repeat(draws, extent[dim] // shards_of).reshape([-1 if axis == dim else 1 for axis in range(len(extent))])
    return level


def normal_values(rng, shape, scale, reach, split=(), kind=jnp.bfloat16):
    entries = jax.random.normal(rng, shape, jnp.float32) * scale
    if len(split) > 0:
        entries = block_scale(rng, shape, split, -0.22, 0.18) * entries
    return jnp.clip(entries, min=-reach, max=reach).astype(kind)


def setup_inputs(seed: int = 0) -> dict:
    key_of = jax.random.split(jax.random.key(seed), 5)
    weights = normal_values(key_of[0], (EXPERTS, ROWS, COLS), 0.5, 3.0, ((0, 16),))
    momentum = normal_values(key_of[1], (REPLICAS, EXPERTS, ROWS, COLS), 1.0, 6.0, ((0, 16), (1, 16)), jnp.float32)
    gradients = normal_values(key_of[2], (STEPS, REPLICAS, EXPERTS, ROWS, COLS), 1.0, 6.0, ((1, 16), (2, 16)))
    outer_momentum = normal_values(key_of[3], (EXPERTS, ROWS, COLS), 0.3, 2.0, ((0, 16), (1, 16)), jnp.float32)
    return dict(weights=weights, momentum=momentum, gradients=gradients, outer_momentum=outer_momentum)


coef_a = 3.4445
coef_b = -4.775
coef_c = 2.0315
inner_beta = 0.9
outer_beta = 0.9
outer_rate = 1.0
epsilon = 1e-07

def dot_high(left, right):
    return jnp.dot(left, right, precision=lax.Precision.HIGHEST, preferred_element_type=jnp.float32)

def orthogonal(matrix):
    norm_value = jnp.sqrt(jnp.sum(matrix * matrix))
    current = (matrix / (norm_value + epsilon)).astype(jnp.bfloat16)
    for index in range(NS_ITERS):
        wide = current.astype(jnp.float32)
        gram = dot_high(wide.T, wide).astype(jnp.bfloat16).astype(jnp.float32)
        poly = (coef_b * gram + coef_c * dot_high(gram, gram)).astype(jnp.bfloat16).astype(jnp.float32)
        current = (coef_a * wide + dot_high(wide, poly)).astype(jnp.bfloat16)
    return current

def per_expert(items):
    start, moment, grads, outer = items
    update_scale = 0.5 * 0.2 * math.sqrt(ROWS)
    local = jnp.broadcast_to(start[None], moment.shape).astype(jnp.bfloat16)
    for step in range(STEPS):
        partner = np.arange(REPLICAS) ^ 1 << step
        moment = inner_beta * moment + grads[step].astype(jnp.float32)
        moment = 0.5 * (moment + moment[partner])
        ortho = lax.map(orthogonal, moment)
        local = (local.astype(jnp.float32) - update_scale * ortho.astype(jnp.float32)).astype(jnp.bfloat16)
    delta = lax.optimization_barrier(jnp.sum(start.astype(jnp.float32)[None] - local.astype(jnp.float32), axis=0)) / REPLICAS
    fresh = outer_beta * outer + delta
    result = (start.astype(jnp.float32) - outer_rate * fresh).astype(jnp.bfloat16)
    return (result, fresh)

def reference(weights, momentum, gradients, outer_momentum):
    moments = jnp.moveaxis(momentum, 1, 0)
    grads = jnp.moveaxis(gradients, 2, 0)
    new_weights, new_outer = lax.map(per_expert, (weights, moments, grads, outer_momentum))
    return (new_weights, new_outer)
```

```python
import functools
import math

import jax
import jax.numpy as jnp
from jax import lax
from jax.experimental import pallas as pl
from jax.experimental.pallas import tpu as pltpu
from jax.sharding import PartitionSpec as P

A, B, C = 3.4445, -4.775, 2.0315
NZ = 8
MESH = pl.DeviceIdType.MESH
F32, BF16 = jnp.float32, jnp.bfloat16

CHUNK = 64
GROUP = 256
LAG = 3

STEPS_0 = (4, 3)
STEPS_1 = (3, 4)
X_ORDER = (4, 5, 3, 6, 2, 7, 1, 0)


def dot(a, b):
    return jnp.dot(a, b, preferred_element_type=F32)


def dot_t(a, b):
    return lax.dot_general(a, b, (((0,), (0,)), ((), ())), preferred_element_type=F32)


def split(a):
    high = a.astype(BF16)
    return high, (a - high.astype(F32)).astype(BF16)


def dot_3(a, b):
    return dot(a[0], b[0]) + dot(a[0], b[1]) + dot(a[1], b[0])


def kernel(
    scale, m_hbm, g_hbm, w_hbm, o_hbm, nw_hbm, no_hbm,
    m_v, g_v, w_v, o_v, no_v, out_v,
    a_in, b_in, a_out, b_out, x0, gram, d0, f_v, norm, e_v, xs, xr, r0, r1, rx,
    load_sem, small_sem, store_sem,
    a_recv, b_recv, ab_send,
    xr_recv, xr_send, r0_recv, r0_send, r1_recv, r1_send, rx_recv, rx_send,
    g0_recv, g0_send, g1_recv, g1_send, gx_recv, gx_send,
):
    rows, cols = m_v.shape
    half = cols // 2
    block = rows // (2 * NZ)
    chunks, groups, per = rows // CHUNK, rows // GROUP, GROUP // CHUNK
    me = lax.axis_index("replica")
    xl, z = me // NZ, lax.rem(me, NZ)
    over = (1 - xl) * NZ + z
    side = xl * NZ

    def at_z(offset):
        return lax.rem(z + offset + NZ, NZ)

    up, down = side + at_z(1), side + at_z(-1)
    q = lax.rem(z, 4)
    edge = jnp.logical_or(q == 0, q == 3)
    pair = side + z + 1 - 2 * lax.rem(z, 2)
    middle = side + lax.rem(jnp.where(q == 1, z + 1, z + NZ - 1), NZ)

    def send(src, dst, send_sem, recv_sem, to):
        return pltpu.make_async_remote_copy(
            src_ref=src, dst_ref=dst, send_sem=send_sem, recv_sem=recv_sem,
            device_id={"replica": to}, device_id_type=MESH,
        )

    def span(i, n):
        return pl.ds(pl.multiple_of(i * n, n), n)

    def load(i):
        s = span(i, GROUP)
        return (
            pltpu.make_async_copy(m_hbm.at[s], m_v.at[s], load_sem.at[0, i]),
            pltpu.make_async_copy(g_hbm.at[0, s], g_v.at[0, s], load_sem.at[1, i]),
            pltpu.make_async_copy(g_hbm.at[1, s], g_v.at[1, s], load_sem.at[2, i]),
        )

    for i in range(groups):
        for c in load(i):
            c.start()
    own_rows = span(me, block)
    small = (
        pltpu.make_async_copy(w_hbm.at[own_rows], w_v, small_sem.at[0]),
        pltpu.make_async_copy(o_hbm, o_v, small_sem.at[1]),
    )
    for c in small:
        c.start()

    barrier = pltpu.get_barrier_semaphore()
    for other in (up, down, over):
        pl.semaphore_signal(barrier, inc=1, device_id={"replica": other}, device_id_type=MESH)
    pl.semaphore_wait(barrier, 3)

    gram[...] = jnp.zeros_like(gram)
    norm[...] = jnp.zeros_like(norm)

    def moment(s):
        return 0.9 * m_v[s, :] + g_v[0, s, :].astype(F32)

    def send_a(i):
        s = span(i, CHUNK)
        return send(a_out.at[s], a_in.at[s], ab_send.at[0], a_recv.at[i], pair)

    def send_b(i):
        s = span(i, CHUNK)
        return send(b_out.at[s], b_in.at[s], ab_send.at[1], b_recv.at[i], middle)

    def keep(s, value):
        x0[s, :] = value.astype(BF16)
        squares = (value * value).reshape(CHUNK // 8, 8, cols)
        norm[...] += jnp.sum(squares, axis=0)

    def add_gram(j):
        x = x0[span(j, GROUP), :]
        gram[...] += dot_t(x, x)

    @pl.when(edge)
    def _():
        @pl.loop(0, groups)
        def _(j):
            for c in load(j):
                c.wait()
            for k in range(per):
                i = j * per + k
                s = span(i, CHUNK)
                a_out[s, :] = moment(s).astype(BF16)
                send_a(i).start()

        @pl.loop(0, groups)
        def _(j):
            for k in range(per):
                i = j * per + k
                s = span(i, CHUNK)
                send_a(i).wait_recv()
                keep(s, a_in[s, :].astype(F32) + 0.225 * moment(s) + 0.5 * g_v[1, s, :].astype(F32))
            add_gram(j)

        send(a_out, a_in, ab_send.at[0], a_recv.at[0], pair).wait_send()

    @pl.when(jnp.logical_not(edge))
    def _():
        def second(i):
            s = span(i, CHUNK)
            send_b(i).wait_recv()
            a_out[s, :] = (b_in[s, :].astype(F32) + 0.225 * moment(s)).astype(BF16)
            send_a(i).start()

        @pl.loop(0, groups)
        def _(j):
            for c in load(j):
                c.wait()
            for k in range(per):
                i = j * per + k
                s = span(i, CHUNK)
                send_a(i).wait_recv()
                mean = 0.5 * (a_in[s, :].astype(F32) + moment(s))
                b_out[s, :] = (0.45 * mean + 0.5 * g_v[1, s, :].astype(F32)).astype(BF16)
                send_b(i).start()
                keep(s, mean)
                if k >= LAG:
                    second(i - LAG)
                else:
                    pl.when(j > 0)(functools.partial(second, i - LAG))
            add_gram(j)

        for i in range(chunks - LAG, chunks):
            second(i)
        send(a_out, a_in, ab_send.at[0], a_recv.at[0], pair).wait_send()
        send(b_out, b_in, ab_send.at[1], b_recv.at[0], middle).wait_send()

    total = jnp.sum(jnp.sum(norm[...], axis=0, keepdims=True), axis=1, keepdims=True)
    unit = 1.0 / (jnp.sqrt(total) + 1e-7)

    g = gram[...] * (unit * unit)
    gs = split(g)
    d = B * g + C * dot(gs[0], gs[0])
    d0[...] = d
    ds = split(d)
    t = dot_3(gs, ds)
    gram[...] = (A * A) * g + (2 * A) * t + dot_3(split(t), ds)

    g = gram[...]
    gh = g.astype(BF16)
    d = B * g + C * dot(gh, gh)
    dh = d.astype(BF16)
    first = d0[...]
    f_v[...] = A * (first + d) + dot(first.astype(BF16), dh)
    t = dot(gh, dh)
    gram[...] = (A * A) * g + (2 * A) * t + dot(t.astype(BF16), dh)

    g = gram[...]
    gh = g.astype(BF16)
    d = B * g + C * dot(gh, gh)
    f = f_v[...]
    e = (A * A) * d + A * f + dot(f.astype(BF16), d.astype(BF16))
    factor = unit * scale
    e_v[...] = (e * factor).astype(BF16)
    lead = factor * (A * A * A)

    def row_block(k):
        return xl * NZ + at_z(k)

    def send_xr(k):
        zz = at_z(k)
        return send(xs.at[0, (1 - xl) * NZ + zz], xr.at[zz], xr_send.at[k], xr_recv.at[k], over)

    def slot(steps, way, t):
        return (0 if way > 0 else steps[0]) + t - 1

    def steps_of(steps, way):
        return steps[0] if way > 0 else steps[1]

    def towards(way):
        return up if way > 0 else down

    def x_of(jj):
        return 1 - xl if jj == 0 else xl

    def send_r0(way, t, src):
        i = slot(STEPS_0, way, t)
        return send(src, r0.at[i], r0_send.at[i], r0_recv.at[i], towards(way))

    def send_r1(jj, way, t, src):
        i = slot(STEPS_1, way, t)
        return send(src, r1.at[jj, i], r1_send.at[jj, i], r1_recv.at[jj, i], towards(way))

    def offset(way, n, t):
        return way * (n + 1 - t)

    sent = []
    e = e_v[...]
    for k in X_ORDER:
        zz = at_z(k)
        x = jnp.concatenate([x0[span(zz, block), :], x0[span(NZ + zz, block), :]], axis=0)
        y = (lead * x.astype(F32) + dot(x, e)).astype(BF16)
        for h in range(2):
            xs[h, zz] = y[:block, h * half : (h + 1) * half]
            xs[h, NZ + zz] = y[block:, h * half : (h + 1) * half]
        sent.append(send_xr(k))
        sent[-1].start()
        for way in (1, -1):
            n = steps_of(STEPS_1, way)
            if (way * n) % NZ == k:
                for jj in range(2):
                    sent.append(send_r1(jj, way, 1, xs.at[1, x_of(jj) * NZ + zz]))
                    sent[-1].start()

    def own_0(k):
        send_xr(k % NZ).wait_recv()
        zz = at_z(k)
        return zz, xs[0, side + zz].astype(F32) + xr[zz].astype(F32)

    def forward_0(way, t):
        n = steps_of(STEPS_0, way)
        i = slot(STEPS_0, way, t)
        send_r0(way, t, r0.at[i]).wait_recv()
        _, own = own_0(offset(way, n, t + 1))
        r0[i] = (r0[i].astype(F32) + own).astype(BF16)
        sent.append(send_r0(way, t + 1, r0.at[i]))
        sent[-1].start()

    def forward_1(jj, way, t):
        n = steps_of(STEPS_1, way)
        i = slot(STEPS_1, way, t)
        send_r1(jj, way, t, r1.at[jj, i]).wait_recv()
        own = xs[1, x_of(jj) * NZ + at_z(offset(way, n, t + 1))]
        r1[jj, i] = (r1[jj, i].astype(F32) + own.astype(F32)).astype(BF16)
        sent.append(send_r1(jj, way, t + 1, r1.at[jj, i]))
        sent[-1].start()

    for way in (1, -1):
        zz, own = own_0(offset(way, steps_of(STEPS_0, way), 1))
        xr[zz] = own.astype(BF16)
        sent.append(send_r0(way, 1, xr.at[zz]))
        sent[-1].start()
    for t in range(1, 4):
        for jj in range(2):
            for way in (1, -1):
                if t < steps_of(STEPS_1, way):
                    forward_1(jj, way, t)
        for way in (1, -1):
            if t < steps_of(STEPS_0, way):
                forward_0(way, t)

    def last_1(jj):
        out = xs[1, x_of(jj) * NZ + z].astype(F32)
        for way in (1, -1):
            i = slot(STEPS_1, way, steps_of(STEPS_1, way))
            send_r1(jj, way, steps_of(STEPS_1, way), r1.at[jj, i]).wait_recv()
            out += r1[jj, i].astype(F32)
        return out

    xs[1, (1 - xl) * NZ + z] = last_1(0).astype(BF16)
    cross = send(xs.at[1, (1 - xl) * NZ + z], rx, rx_send, rx_recv, over)
    cross.start()

    _, sum_0 = own_0(0)
    for way in (1, -1):
        n = steps_of(STEPS_0, way)
        i = slot(STEPS_0, way, n)
        send_r0(way, n, r0.at[i]).wait_recv()
        sum_0 += r0[i].astype(F32)

    for c in small:
        c.wait()

    def piece(b, h):
        return out_v.at[span(b, block), pl.ds(h * half, half)]

    def outer(h, delta):
        c = pl.ds(h * half, half)
        fresh = 0.9 * o_v[:, c] + delta
        no_v[:, c] = fresh
        out_v[own_rows, c] = (w_v[:, c].astype(F32) - fresh).astype(BF16)

    def send_g0(way, t):
        i = slot(STEPS_0, way, t)
        p = piece(side + at_z(-way * (t - 1)), 0)
        return send(p, p, g0_send.at[i], g0_recv.at[i], towards(way))

    def got_g0(way, t):
        i = slot(STEPS_0, way, t)
        p = piece(side + at_z(-way * t), 0)
        send(p, p, g0_send.at[i], g0_recv.at[i], towards(way)).wait_recv()

    def send_gx(k):
        p = piece(row_block(k), 0)
        return send(p, p, gx_send.at[k], gx_recv.at[k], over)

    def got_gx(k):
        p = piece((1 - xl) * NZ + at_z(k), 0)
        send(p, p, gx_send.at[k], gx_recv.at[k], over).wait_recv()

    def send_g1(jj, way, t):
        i = slot(STEPS_1, way, t)
        p = piece(x_of(jj) * NZ + at_z(-way * (t - 1)), 1)
        return send(p, p, g1_send.at[jj, i], g1_recv.at[jj, i], towards(way))

    def got_g1(jj, way, t):
        i = slot(STEPS_1, way, t)
        p = piece(x_of(jj) * NZ + at_z(-way * t), 1)
        send(p, p, g1_send.at[jj, i], g1_recv.at[jj, i], towards(way)).wait_recv()

    def go(c):
        sent.append(c)
        c.start()

    outer(0, sum_0)
    for way in (1, -1):
        go(send_g0(way, 1))
    go(send_gx(0))

    sum_1 = last_1(1)
    cross.wait_recv()
    outer(1, sum_1 + rx[...].astype(F32))
    p = piece(me, 1)
    go(send(p, p, gx_send.at[NZ], gx_recv.at[NZ], over))
    for way in (1, -1):
        go(send_g1(1, way, 1))
    store_outer = pltpu.make_async_copy(no_v, no_hbm, small_sem.at[2])
    store_outer.start()
    p = piece(over, 1)
    send(p, p, gx_send.at[NZ], gx_recv.at[NZ], over).wait_recv()
    for way in (1, -1):
        go(send_g1(0, way, 1))

    for t in range(1, 5):
        for way in (1, -1):
            n = steps_of(STEPS_0, way)
            if t <= n:
                got_g0(way, t)
                if t < n:
                    go(send_g0(way, t + 1))
                go(send_gx((-way * t) % NZ))
        for jj in (1, 0):
            for way in (1, -1):
                n = steps_of(STEPS_1, way)
                if t <= n:
                    got_g1(jj, way, t)
                    if t < n:
                        go(send_g1(jj, way, t + 1))
    for k in range(NZ):
        got_gx(k)

    store = pltpu.make_async_copy(out_v, nw_hbm, store_sem)
    store.start()
    for c in sent:
        c.wait_send()
    cross.wait_send()
    store_outer.wait()
    store.wait()


def per_device(weights, momentum, gradients, outer_momentum):
    rows, cols = weights.shape[1:]
    half, block = cols // 2, rows // (2 * NZ)
    chunks, groups = rows // CHUNK, rows // GROUP
    scale = 2 * 0.5 * 0.2 * math.sqrt(rows) / (2 * NZ)
    any_spec = pl.BlockSpec(memory_space=pl.ANY)
    dma = pltpu.SemaphoreType.DMA
    new_weights, new_outer = pl.pallas_call(
        functools.partial(kernel, scale),
        out_shape=(
            jax.ShapeDtypeStruct((rows, cols), BF16),
            jax.ShapeDtypeStruct((block, cols), F32),
        ),
        in_specs=[any_spec] * 4,
        out_specs=(any_spec, any_spec),
        scratch_shapes=[
            pltpu.VMEM((rows, cols), F32),
            pltpu.VMEM((2, rows, cols), BF16),
            pltpu.VMEM((block, cols), BF16),
            pltpu.VMEM((block, cols), F32),
            pltpu.VMEM((block, cols), F32),
            pltpu.VMEM((rows, cols), BF16),
            pltpu.VMEM((rows, cols), BF16),
            pltpu.VMEM((rows, cols), BF16),
            pltpu.VMEM((rows, cols), BF16),
            pltpu.VMEM((rows, cols), BF16),
            pltpu.VMEM((rows, cols), BF16),
            pltpu.VMEM((cols, cols), F32),
            pltpu.VMEM((cols, cols), F32),
            pltpu.VMEM((cols, cols), F32),
            pltpu.VMEM((8, cols), F32),
            pltpu.VMEM((cols, cols), BF16),
            pltpu.VMEM((2, 2 * NZ, block, half), BF16),
            pltpu.VMEM((NZ, block, half), BF16),
            pltpu.VMEM((NZ - 1, block, half), BF16),
            pltpu.VMEM((2, NZ - 1, block, half), BF16),
            pltpu.VMEM((block, half), BF16),
            dma((3, groups)),
            dma((3,)),
            dma,
            dma((chunks,)), dma((chunks,)), dma((2,)),
            dma((NZ,)), dma((NZ,)),
            dma((NZ - 1,)), dma((NZ - 1,)),
            dma((2, NZ - 1)), dma((2, NZ - 1)),
            dma, dma,
            dma((NZ - 1,)), dma((NZ - 1,)),
            dma((2, NZ - 1)), dma((2, NZ - 1)),
            dma((NZ + 1,)), dma((NZ + 1,)),
        ],
        compiler_params=pltpu.CompilerParams(
            collective_id=0, has_side_effects=True, vmem_limit_bytes=56 * 1024 * 1024
        ),
        name="gossip_muon",
    )(momentum[0, 0], gradients[:, 0, 0], weights[0], outer_momentum[0])
    return new_weights[None], new_outer[None]


def solution(mesh):
    return jax.shard_map(
        per_device,
        mesh=mesh,
        in_specs=(
            P("expert", None, None),
            P("replica", "expert", None, None),
            P(None, "replica", "expert", None, None),
            P("expert", "replica", None),
        ),
        out_specs=(P("expert", None, None), P("expert", "replica", None)),
        check_vma=False,
    )
```

```python
import functools
import math

import jax
import jax.numpy as jnp
from jax import lax
from jax.experimental import pallas as pl
from jax.experimental.pallas import tpu as pltpu
from jax.sharding import PartitionSpec as P

A, B, C = 3.4445, -4.775, 2.0315
NZ = 8
MESH = pl.DeviceIdType.MESH
F32, BF16 = jnp.float32, jnp.bfloat16

CHUNK = 32
GROUP = 256
LAG = 4

STEPS_0 = (4, 3)
STEPS_1 = (3, 4)
X_ORDER = (4, 5, 3, 6, 2, 7, 1, 0)


def dot(a, b):
    return jnp.dot(a, b, preferred_element_type=F32)


def dot_t(a, b):
    return lax.dot_general(a, b, (((0,), (0,)), ((), ())), preferred_element_type=F32)


def kernel(
    scale, m_hbm, g_hbm, w_hbm, o_hbm, out_v, no_v,
    m_v, g_v, w_v, o_v,
    a_in, b_in, a_out, b_out, x0, gram, d0, f_v, norm, e_v, xs, xr, r0, r1, rx,
    load_sem, small_sem,
    a_recv, b_recv, ab_send,
    xr_recv, xr_send, r0_recv, r0_send, r1_recv, r1_send, rx_recv, rx_send,
    g0_recv, g0_send, g1_recv, g1_send, gx_recv, gx_send,
):
    rows, cols = m_v.shape
    half = cols // 2
    block = rows // (2 * NZ)
    chunks, groups, per = rows // CHUNK, rows // GROUP, GROUP // CHUNK
    me = lax.axis_index("replica")
    xl, z = me // NZ, lax.rem(me, NZ)
    over = (1 - xl) * NZ + z
    side = xl * NZ

    def at_z(offset):
        return lax.rem(z + offset + NZ, NZ)

    up, down = side + at_z(1), side + at_z(-1)
    q = lax.rem(z, 4)
    edge = jnp.logical_or(q == 0, q == 3)
    pair = side + z + 1 - 2 * lax.rem(z, 2)
    middle = side + lax.rem(jnp.where(q == 1, z + 1, z + NZ - 1), NZ)

    def send(src, dst, send_sem, recv_sem, to):
        return pltpu.make_async_remote_copy(
            src_ref=src, dst_ref=dst, send_sem=send_sem, recv_sem=recv_sem,
            device_id={"replica": to}, device_id_type=MESH,
        )

    def span(i, n):
        return pl.ds(pl.multiple_of(i * n, n), n)

    def load(i):
        s = span(i, GROUP)
        return (
            pltpu.make_async_copy(m_hbm.at[s], m_v.at[s], load_sem.at[0, i]),
            pltpu.make_async_copy(g_hbm.at[0, s], g_v.at[0, s], load_sem.at[1, i]),
            pltpu.make_async_copy(g_hbm.at[1, s], g_v.at[1, s], load_sem.at[2, i]),
        )

    for i in range(groups):
        for c in load(i):
            c.start()
    own_rows = span(me, block)
    small = (
        pltpu.make_async_copy(w_hbm.at[own_rows], w_v, small_sem.at[0]),
        pltpu.make_async_copy(o_hbm, o_v, small_sem.at[1]),
    )
    for c in small:
        c.start()

    barrier = pltpu.get_barrier_semaphore()
    for other in (up, down, over):
        pl.semaphore_signal(barrier, inc=1, device_id={"replica": other}, device_id_type=MESH)
    pl.semaphore_wait(barrier, 3)

    gram[...] = jnp.zeros_like(gram)
    norm[...] = jnp.zeros_like(norm)

    def moment(s):
        return 0.9 * m_v[s, :] + g_v[0, s, :].astype(F32)

    def send_a(i):
        s = span(i, CHUNK)
        return send(a_out.at[s], a_in.at[s], ab_send.at[0], a_recv.at[i], pair)

    def send_b(i):
        s = span(i, CHUNK)
        return send(b_out.at[s], b_in.at[s], ab_send.at[1], b_recv.at[i], middle)

    def keep(s, value):
        x0[s, :] = value.astype(BF16)
        squares = (value * value).reshape(CHUNK // 8, 8, cols)
        norm[...] += jnp.sum(squares, axis=0)

    def add_gram(j):
        x = x0[span(j, GROUP), :]
        gram[...] += dot_t(x, x)

    @pl.when(edge)
    def _():
        @pl.loop(0, groups)
        def _(j):
            for c in load(j):
                c.wait()
            for k in range(per):
                i = j * per + k
                s = span(i, CHUNK)
                a_out[s, :] = moment(s).astype(BF16)
                send_a(i).start()

        @pl.loop(0, groups)
        def _(j):
            for k in range(per):
                i = j * per + k
                s = span(i, CHUNK)
                send_a(i).wait_recv()
                keep(s, a_in[s, :].astype(F32) + 0.225 * moment(s) + 0.5 * g_v[1, s, :].astype(F32))
            add_gram(j)

    @pl.when(jnp.logical_not(edge))
    def _():
        def second(i):
            s = span(i, CHUNK)
            send_b(i).wait_recv()
            a_out[s, :] = (b_in[s, :].astype(F32) + 0.225 * moment(s)).astype(BF16)
            send_a(i).start()

        @pl.loop(0, groups)
        def _(j):
            for c in load(j):
                c.wait()
            for k in range(per):
                i = j * per + k
                s = span(i, CHUNK)
                send_a(i).wait_recv()
                mean = 0.5 * (a_in[s, :].astype(F32) + moment(s))
                b_out[s, :] = (0.45 * mean + 0.5 * g_v[1, s, :].astype(F32)).astype(BF16)
                send_b(i).start()
                keep(s, mean)
                if k >= LAG:
                    second(i - LAG)
                else:
                    pl.when(j > 0)(functools.partial(second, i - LAG))
            add_gram(j)

        for i in range(chunks - LAG, chunks):
            second(i)

    total = jnp.sum(jnp.sum(norm[...], axis=0, keepdims=True), axis=1, keepdims=True)
    unit = 1.0 / (jnp.sqrt(total) + 1e-7)

    g = gram[...] * (unit * unit)
    gh = g.astype(BF16)
    d = B * g + C * dot(gh, gh)
    d0[...] = d
    dh = d.astype(BF16)
    t = dot(gh, dh)
    gram[...] = (A * A) * g + (2 * A) * t + dot(t.astype(BF16), dh)

    g = gram[...]
    gh = g.astype(BF16)
    d = B * g + C * dot(gh, gh)
    dh = d.astype(BF16)
    first = d0[...]
    f_v[...] = A * (first + d) + dot(first.astype(BF16), dh)
    t = dot(gh, dh)
    gram[...] = (A * A) * g + (2 * A) * t + dot(t.astype(BF16), dh)

    g = gram[...]
    gh = g.astype(BF16)
    d = B * g + C * dot(gh, gh)
    f = f_v[...]
    e = (A * A) * d + A * f + dot(f.astype(BF16), d.astype(BF16))
    factor = unit * scale
    e_v[...] = (e * factor).astype(BF16)
    lead = factor * (A * A * A)

    def row_block(k):
        return xl * NZ + at_z(k)

    def send_xr(k):
        zz = at_z(k)
        return send(xs.at[0, (1 - xl) * NZ + zz], xr.at[zz], xr_send.at[k], xr_recv.at[k], over)

    def slot(steps, way, t):
        return (0 if way > 0 else steps[0]) + t - 1

    def steps_of(steps, way):
        return steps[0] if way > 0 else steps[1]

    def towards(way):
        return up if way > 0 else down

    def x_of(jj):
        return 1 - xl if jj == 0 else xl

    def send_r0(way, t, src):
        i = slot(STEPS_0, way, t)
        return send(src, r0.at[i], r0_send.at[i], r0_recv.at[i], towards(way))

    def send_r1(jj, way, t, src):
        i = slot(STEPS_1, way, t)
        return send(src, r1.at[jj, i], r1_send.at[jj, i], r1_recv.at[jj, i], towards(way))

    def offset(way, n, t):
        return way * (n + 1 - t)

    sent = []
    e = e_v[...]
    for k in X_ORDER:
        zz = at_z(k)
        x = jnp.concatenate([x0[span(zz, block), :], x0[span(NZ + zz, block), :]], axis=0)
        y = (lead * x.astype(F32) + dot(x, e)).astype(BF16)
        for h in range(2):
            xs[h, zz] = y[:block, h * half : (h + 1) * half]
            xs[h, NZ + zz] = y[block:, h * half : (h + 1) * half]
        sent.append(send_xr(k))
        sent[-1].start()
        for way in (1, -1):
            n = steps_of(STEPS_1, way)
            if (way * n) % NZ == k:
                for jj in range(2):
                    sent.append(send_r1(jj, way, 1, xs.at[1, x_of(jj) * NZ + zz]))
                    sent[-1].start()

    def own_0(k):
        send_xr(k % NZ).wait_recv()
        zz = at_z(k)
        return zz, xs[0, side + zz].astype(F32) + xr[zz].astype(F32)

    def forward_0(way, t):
        n = steps_of(STEPS_0, way)
        i = slot(STEPS_0, way, t)
        send_r0(way, t, r0.at[i]).wait_recv()
        _, own = own_0(offset(way, n, t + 1))
        r0[i] = (r0[i].astype(F32) + own).astype(BF16)
        sent.append(send_r0(way, t + 1, r0.at[i]))
        sent[-1].start()

    def forward_1(jj, way, t):
        n = steps_of(STEPS_1, way)
        i = slot(STEPS_1, way, t)
        send_r1(jj, way, t, r1.at[jj, i]).wait_recv()
        own = xs[1, x_of(jj) * NZ + at_z(offset(way, n, t + 1))]
        r1[jj, i] = (r1[jj, i].astype(F32) + own.astype(F32)).astype(BF16)
        sent.append(send_r1(jj, way, t + 1, r1.at[jj, i]))
        sent[-1].start()

    for way in (1, -1):
        zz, own = own_0(offset(way, steps_of(STEPS_0, way), 1))
        xr[zz] = own.astype(BF16)
        sent.append(send_r0(way, 1, xr.at[zz]))
        sent[-1].start()
    for t in range(1, 4):
        for jj in range(2):
            for way in (1, -1):
                if t < steps_of(STEPS_1, way):
                    forward_1(jj, way, t)
        for way in (1, -1):
            if t < steps_of(STEPS_0, way):
                forward_0(way, t)

    def last_1(jj):
        out = xs[1, x_of(jj) * NZ + z].astype(F32)
        for way in (1, -1):
            i = slot(STEPS_1, way, steps_of(STEPS_1, way))
            send_r1(jj, way, steps_of(STEPS_1, way), r1.at[jj, i]).wait_recv()
            out += r1[jj, i].astype(F32)
        return out

    xs[1, (1 - xl) * NZ + z] = last_1(0).astype(BF16)
    cross = send(xs.at[1, (1 - xl) * NZ + z], rx, rx_send, rx_recv, over)
    cross.start()

    _, sum_0 = own_0(0)
    for way in (1, -1):
        n = steps_of(STEPS_0, way)
        i = slot(STEPS_0, way, n)
        send_r0(way, n, r0.at[i]).wait_recv()
        sum_0 += r0[i].astype(F32)

    for c in small:
        c.wait()

    def piece(b, h):
        return out_v.at[span(b, block), pl.ds(h * half, half)]

    def outer(h, delta):
        c = pl.ds(h * half, half)
        fresh = 0.9 * o_v[:, c] + delta
        no_v[:, c] = fresh
        out_v[own_rows, c] = (w_v[:, c].astype(F32) - fresh).astype(BF16)

    def send_g0(way, t):
        i = slot(STEPS_0, way, t)
        p = piece(side + at_z(-way * (t - 1)), 0)
        return send(p, p, g0_send.at[i], g0_recv.at[i], towards(way))

    def got_g0(way, t):
        i = slot(STEPS_0, way, t)
        p = piece(side + at_z(-way * t), 0)
        send(p, p, g0_send.at[i], g0_recv.at[i], towards(way)).wait_recv()

    def send_gx(k):
        p = piece(row_block(k), 0)
        return send(p, p, gx_send.at[k], gx_recv.at[k], over)

    def got_gx(k):
        p = piece((1 - xl) * NZ + at_z(k), 0)
        send(p, p, gx_send.at[k], gx_recv.at[k], over).wait_recv()

    def send_g1(jj, way, t):
        i = slot(STEPS_1, way, t)
        p = piece(x_of(jj) * NZ + at_z(-way * (t - 1)), 1)
        return send(p, p, g1_send.at[jj, i], g1_recv.at[jj, i], towards(way))

    def got_g1(jj, way, t):
        i = slot(STEPS_1, way, t)
        p = piece(x_of(jj) * NZ + at_z(-way * t), 1)
        send(p, p, g1_send.at[jj, i], g1_recv.at[jj, i], towards(way)).wait_recv()

    def go(c):
        sent.append(c)
        c.start()

    outer(0, sum_0)
    for way in (1, -1):
        go(send_g0(way, 1))
    go(send_gx(0))

    sum_1 = last_1(1)
    cross.wait_recv()
    outer(1, sum_1 + rx[...].astype(F32))
    p = piece(me, 1)
    go(send(p, p, gx_send.at[NZ], gx_recv.at[NZ], over))
    for way in (1, -1):
        go(send_g1(1, way, 1))
    p = piece(over, 1)
    send(p, p, gx_send.at[NZ], gx_recv.at[NZ], over).wait_recv()
    for way in (1, -1):
        go(send_g1(0, way, 1))

    for t in range(1, 5):
        for way in (1, -1):
            n = steps_of(STEPS_0, way)
            if t <= n:
                got_g0(way, t)
                if t < n:
                    go(send_g0(way, t + 1))
                go(send_gx((-way * t) % NZ))
        for jj in (1, 0):
            for way in (1, -1):
                n = steps_of(STEPS_1, way)
                if t <= n:
                    got_g1(jj, way, t)
                    if t < n:
                        go(send_g1(jj, way, t + 1))
    for k in range(NZ):
        got_gx(k)

    for c in sent:
        c.wait_send()
    cross.wait_send()
    send(a_out, a_in, ab_send.at[0], a_recv.at[0], pair).wait_send()

    @pl.when(jnp.logical_not(edge))
    def _():
        send(b_out, b_in, ab_send.at[1], b_recv.at[0], middle).wait_send()


def write_out(w_v, o_v, w_hbm, o_hbm, sem):
    copies = (
        pltpu.make_async_copy(w_v, w_hbm, sem.at[0]),
        pltpu.make_async_copy(o_v, o_hbm, sem.at[1]),
    )
    for c in copies:
        c.start()
    for c in copies:
        c.wait()


def per_device(weights, momentum, gradients, outer_momentum):
    rows, cols = weights.shape[1:]
    half, block = cols // 2, rows // (2 * NZ)
    chunks, groups = rows // CHUNK, rows // GROUP
    scale = 2 * 0.5 * 0.2 * math.sqrt(rows) / (2 * NZ)
    hbm_spec = pl.BlockSpec(memory_space=pltpu.HBM)
    any_spec = pl.BlockSpec(memory_space=pl.ANY)
    vmem_spec = pl.BlockSpec(memory_space=pltpu.VMEM)
    dma = pltpu.SemaphoreType.DMA
    new_weights, new_outer = pl.pallas_call(
        functools.partial(kernel, scale),
        out_shape=(pltpu.VMEM((rows, cols), BF16), pltpu.VMEM((block, cols), F32)),
        in_specs=[hbm_spec] * 4,
        out_specs=(vmem_spec, vmem_spec),
        scratch_shapes=[
            pltpu.VMEM((rows, cols), F32),
            pltpu.VMEM((2, rows, cols), BF16),
            pltpu.VMEM((block, cols), BF16),
            pltpu.VMEM((block, cols), F32),
            pltpu.VMEM((rows, cols), BF16),
            pltpu.VMEM((rows, cols), BF16),
            pltpu.VMEM((rows, cols), BF16),
            pltpu.VMEM((rows, cols), BF16),
            pltpu.VMEM((rows, cols), BF16),
            pltpu.VMEM((cols, cols), F32),
            pltpu.VMEM((cols, cols), F32),
            pltpu.VMEM((cols, cols), F32),
            pltpu.VMEM((8, cols), F32),
            pltpu.VMEM((cols, cols), BF16),
            pltpu.VMEM((2, 2 * NZ, block, half), BF16),
            pltpu.VMEM((NZ, block, half), BF16),
            pltpu.VMEM((NZ - 1, block, half), BF16),
            pltpu.VMEM((2, NZ - 1, block, half), BF16),
            pltpu.VMEM((block, half), BF16),
            dma((3, groups)),
            dma((2,)),
            dma((chunks,)), dma((chunks,)), dma((2,)),
            dma((NZ,)), dma((NZ,)),
            dma((NZ - 1,)), dma((NZ - 1,)),
            dma((2, NZ - 1)), dma((2, NZ - 1)),
            dma, dma,
            dma((NZ - 1,)), dma((NZ - 1,)),
            dma((2, NZ - 1)), dma((2, NZ - 1)),
            dma((NZ + 1,)), dma((NZ + 1,)),
        ],
        compiler_params=pltpu.CompilerParams(
            collective_id=0, has_side_effects=True, vmem_limit_bytes=48 * 1024 * 1024
        ),
        name="gossip_muon",
    )(*(
        pltpu.with_memory_space_constraint(a, pltpu.HBM)
        for a in (momentum[0, 0], gradients[:, 0, 0], weights[0], outer_momentum[0])
    ))
    new_weights, new_outer = pl.pallas_call(
        write_out,
        out_shape=(
            jax.ShapeDtypeStruct((rows, cols), BF16),
            jax.ShapeDtypeStruct((block, cols), F32),
        ),
        in_specs=[vmem_spec] * 2,
        out_specs=(any_spec, any_spec),
        scratch_shapes=[dma((2,))],
        name="write_out",
    )(
        pltpu.with_memory_space_constraint(new_weights, pltpu.VMEM),
        pltpu.with_memory_space_constraint(new_outer, pltpu.VMEM),
    )
    return new_weights[None], new_outer[None]


def solution(mesh):
    return jax.shard_map(
        per_device,
        mesh=mesh,
        in_specs=(
            P("expert", None, None),
            P("replica", "expert", None, None),
            P(None, "replica", "expert", None, None),
            P("expert", "replica", None),
        ),
        out_specs=(P("expert", None, None), P("expert", "replica", None)),
        check_vma=False,
    )
```

```python
import functools
import math

import jax
import jax.numpy as jnp
from jax import lax
from jax.experimental import pallas as pl
from jax.experimental.pallas import tpu as pltpu
from jax.sharding import PartitionSpec as P

A, B, C = 3.4445, -4.775, 2.0315
NZ = 8
MESH = pl.DeviceIdType.MESH
F32, BF16 = jnp.float32, jnp.bfloat16

CHUNK = 32
GROUP = 256
LAG = 4

STEPS_0 = (4, 3)
STEPS_1 = (3, 4)
WAVES = 2
X_ORDER = (4, 5, 3, 6, 2, 7, 1, 0)


def dot(a, b):
    return jnp.dot(a, b, preferred_element_type=F32)


def dot_t(a, b):
    return lax.dot_general(a, b, (((0,), (0,)), ((), ())), preferred_element_type=F32)


def kernel(
    scale, m_hbm, g_hbm, w_hbm, o_hbm, out_v, no_v,
    m_v, g_v, w_v, o_v,
    a_in, b_in, a_out, b_out, x0, gram, d0, f_v, norm, e_v, xs, xr, r0, r1, rx,
    load_sem, small_sem,
    a_recv, b_recv, ab_send,
    xr_recv, xr_send, r0_recv, r0_send, r1_recv, r1_send, rx_recv, rx_send,
    g0_recv, g0_send, g1_recv, g1_send, gx_recv, gx_send,
):
    rows, cols = m_v.shape
    half = cols // 2
    block = rows // (2 * NZ)
    part = block // WAVES
    chunks, groups, per = rows // CHUNK, rows // GROUP, GROUP // CHUNK
    me = lax.axis_index("replica")
    xl, z = me // NZ, lax.rem(me, NZ)
    over = (1 - xl) * NZ + z
    side = xl * NZ

    def at_z(offset):
        return lax.rem(z + offset + NZ, NZ)

    up, down = side + at_z(1), side + at_z(-1)
    q = lax.rem(z, 4)
    edge = jnp.logical_or(q == 0, q == 3)
    pair = side + z + 1 - 2 * lax.rem(z, 2)
    middle = side + lax.rem(jnp.where(q == 1, z + 1, z + NZ - 1), NZ)

    def send(src, dst, send_sem, recv_sem, to):
        return pltpu.make_async_remote_copy(
            src_ref=src, dst_ref=dst, send_sem=send_sem, recv_sem=recv_sem,
            device_id={"replica": to}, device_id_type=MESH,
        )

    def span(i, n):
        return pl.ds(pl.multiple_of(i * n, n), n)

    def load(i):
        s = span(i, GROUP)
        return (
            pltpu.make_async_copy(m_hbm.at[s], m_v.at[s], load_sem.at[0, i]),
            pltpu.make_async_copy(g_hbm.at[0, s], g_v.at[0, s], load_sem.at[1, i]),
            pltpu.make_async_copy(g_hbm.at[1, s], g_v.at[1, s], load_sem.at[2, i]),
        )

    for i in range(groups):
        for c in load(i):
            c.start()
    own_rows = span(me, block)
    small = (
        pltpu.make_async_copy(w_hbm.at[own_rows], w_v, small_sem.at[0]),
        pltpu.make_async_copy(o_hbm, o_v, small_sem.at[1]),
    )
    for c in small:
        c.start()

    barrier = pltpu.get_barrier_semaphore()
    for other in (up, down, over):
        pl.semaphore_signal(barrier, inc=1, device_id={"replica": other}, device_id_type=MESH)
    pl.semaphore_wait(barrier, 3)

    gram[...] = jnp.zeros_like(gram)
    norm[...] = jnp.zeros_like(norm)

    def moment(s):
        return 0.9 * m_v[s, :] + g_v[0, s, :].astype(F32)

    def send_a(i):
        s = span(i, CHUNK)
        return send(a_out.at[s], a_in.at[s], ab_send.at[0], a_recv.at[i], pair)

    def send_b(i):
        s = span(i, CHUNK)
        return send(b_out.at[s], b_in.at[s], ab_send.at[1], b_recv.at[i], middle)

    def keep(s, value):
        x0[s, :] = value.astype(BF16)
        squares = (value * value).reshape(CHUNK // 8, 8, cols)
        norm[...] += jnp.sum(squares, axis=0)

    def add_gram(j):
        x = x0[span(j, GROUP), :]
        gram[...] += dot_t(x, x)

    @pl.when(edge)
    def _():
        @pl.loop(0, groups)
        def _(j):
            for c in load(j):
                c.wait()
            for k in range(per):
                i = j * per + k
                s = span(i, CHUNK)
                a_out[s, :] = moment(s).astype(BF16)
                send_a(i).start()

        @pl.loop(0, groups)
        def _(j):
            for k in range(per):
                i = j * per + k
                s = span(i, CHUNK)
                send_a(i).wait_recv()
                keep(s, a_in[s, :].astype(F32) + 0.225 * moment(s) + 0.5 * g_v[1, s, :].astype(F32))
            add_gram(j)

    @pl.when(jnp.logical_not(edge))
    def _():
        def second(i):
            s = span(i, CHUNK)
            send_b(i).wait_recv()
            a_out[s, :] = (b_in[s, :].astype(F32) + 0.225 * moment(s)).astype(BF16)
            send_a(i).start()

        @pl.loop(0, groups)
        def _(j):
            for c in load(j):
                c.wait()
            for k in range(per):
                i = j * per + k
                s = span(i, CHUNK)
                send_a(i).wait_recv()
                mean = 0.5 * (a_in[s, :].astype(F32) + moment(s))
                b_out[s, :] = (0.45 * mean + 0.5 * g_v[1, s, :].astype(F32)).astype(BF16)
                send_b(i).start()
                keep(s, mean)
                if k >= LAG:
                    second(i - LAG)
                else:
                    pl.when(j > 0)(functools.partial(second, i - LAG))
            add_gram(j)

        for i in range(chunks - LAG, chunks):
            second(i)

    total = jnp.sum(jnp.sum(norm[...], axis=0, keepdims=True), axis=1, keepdims=True)
    unit = 1.0 / (jnp.sqrt(total) + 1e-7)

    g = gram[...] * (unit * unit)
    gh = g.astype(BF16)
    d = B * g + C * dot(gh, gh)
    d0[...] = d
    dh = d.astype(BF16)
    t = dot(gh, dh)
    gram[...] = (A * A) * g + (2 * A) * t + dot(t.astype(BF16), dh)

    g = gram[...]
    gh = g.astype(BF16)
    d = B * g + C * dot(gh, gh)
    dh = d.astype(BF16)
    first = d0[...]
    f_v[...] = A * (first + d) + dot(first.astype(BF16), dh)
    t = dot(gh, dh)
    gram[...] = (A * A) * g + (2 * A) * t + dot(t.astype(BF16), dh)

    g = gram[...]
    gh = g.astype(BF16)
    d = B * g + C * dot(gh, gh)
    f = f_v[...]
    e = (A * A) * d + A * f + dot(f.astype(BF16), d.astype(BF16))
    factor = unit * scale
    e_v[...] = (e * factor).astype(BF16)
    lead = factor * (A * A * A)

    def send_xr(v, k):
        zz = at_z(k)
        src = xs.at[0, v, (1 - xl) * NZ + zz]
        return send(src, xr.at[v, zz], xr_send.at[v, k], xr_recv.at[v, k], over)

    def slot(steps, way, t):
        return (0 if way > 0 else steps[0]) + t - 1

    def steps_of(steps, way):
        return steps[0] if way > 0 else steps[1]

    def towards(way):
        return up if way > 0 else down

    def x_of(jj):
        return 1 - xl if jj == 0 else xl

    def send_r0(v, way, t, src):
        i = slot(STEPS_0, way, t)
        return send(src, r0.at[v, i], r0_send.at[v, i], r0_recv.at[v, i], towards(way))

    def send_r1(v, jj, way, t, src):
        i = slot(STEPS_1, way, t)
        return send(src, r1.at[v, jj, i], r1_send.at[v, jj, i], r1_recv.at[v, jj, i], towards(way))

    def offset(way, n, t):
        return way * (n + 1 - t)

    sent = []

    def go(c):
        sent.append(c)
        c.start()

    e = e_v[...]
    for k in X_ORDER:
        zz = at_z(k)
        x = jnp.concatenate([x0[span(zz, block), :], x0[span(NZ + zz, block), :]], axis=0)
        y = (lead * x.astype(F32) + dot(x, e)).astype(BF16)
        for v in range(WAVES):
            for h in range(2):
                c = slice(h * half, (h + 1) * half)
                xs[h, v, zz] = y[v * part : (v + 1) * part, c]
                xs[h, v, NZ + zz] = y[block + v * part : block + (v + 1) * part, c]
        for v in range(WAVES):
            go(send_xr(v, k))
            for way in (1, -1):
                n = steps_of(STEPS_1, way)
                if (way * n) % NZ == k:
                    for jj in range(2):
                        go(send_r1(v, jj, way, 1, xs.at[1, v, x_of(jj) * NZ + zz]))

    def own_0(v, k):
        send_xr(v, k % NZ).wait_recv()
        zz = at_z(k)
        return zz, xs[0, v, side + zz].astype(F32) + xr[v, zz].astype(F32)

    def first_0(v):
        for way in (1, -1):
            zz, own = own_0(v, offset(way, steps_of(STEPS_0, way), 1))
            xr[v, zz] = own.astype(BF16)
            go(send_r0(v, way, 1, xr.at[v, zz]))

    def forward_0(v, way, t):
        n = steps_of(STEPS_0, way)
        i = slot(STEPS_0, way, t)
        send_r0(v, way, t, r0.at[v, i]).wait_recv()
        _, own = own_0(v, offset(way, n, t + 1))
        r0[v, i] = (r0[v, i].astype(F32) + own).astype(BF16)
        go(send_r0(v, way, t + 1, r0.at[v, i]))

    def forward_1(v, jj, way, t):
        n = steps_of(STEPS_1, way)
        i = slot(STEPS_1, way, t)
        send_r1(v, jj, way, t, r1.at[v, jj, i]).wait_recv()
        own = xs[1, v, x_of(jj) * NZ + at_z(offset(way, n, t + 1))]
        r1[v, jj, i] = (r1[v, jj, i].astype(F32) + own.astype(F32)).astype(BF16)
        go(send_r1(v, jj, way, t + 1, r1.at[v, jj, i]))

    def reduce_step(v, t):
        for jj in range(2):
            for way in (1, -1):
                if t < steps_of(STEPS_1, way):
                    forward_1(v, jj, way, t)
        for way in (1, -1):
            if t < steps_of(STEPS_0, way):
                forward_0(v, way, t)

    def last_1(v, jj):
        out = xs[1, v, x_of(jj) * NZ + z].astype(F32)
        for way in (1, -1):
            n = steps_of(STEPS_1, way)
            i = slot(STEPS_1, way, n)
            send_r1(v, jj, way, n, r1.at[v, jj, i]).wait_recv()
            out += r1[v, jj, i].astype(F32)
        return out

    def last_0(v):
        _, out = own_0(v, 0)
        for way in (1, -1):
            n = steps_of(STEPS_0, way)
            i = slot(STEPS_0, way, n)
            send_r0(v, way, n, r0.at[v, i]).wait_recv()
            out += r0[v, i].astype(F32)
        return out

    def cross(v):
        src = xs.at[1, v, (1 - xl) * NZ + z]
        return send(src, rx.at[v], rx_send.at[v], rx_recv.at[v], over)

    def rows_of(v, b):
        return pl.ds(pl.multiple_of(b * block + v * part, part), part)

    def piece(v, b, h):
        return out_v.at[rows_of(v, b), pl.ds(h * half, half)]

    def outer(v, h, delta):
        r, c = slice(v * part, (v + 1) * part), slice(h * half, (h + 1) * half)
        fresh = 0.9 * o_v[r, c] + delta
        no_v[r, c] = fresh
        out_v[rows_of(v, me), c] = (w_v[r, c].astype(F32) - fresh).astype(BF16)

    def send_g0(v, way, t, p):
        i = slot(STEPS_0, way, t)
        return send(p, p, g0_send.at[v, i], g0_recv.at[v, i], towards(way))

    def send_g1(v, jj, way, t, p):
        i = slot(STEPS_1, way, t)
        return send(p, p, g1_send.at[v, jj, i], g1_recv.at[v, jj, i], towards(way))

    def send_gx(v, k, p):
        return send(p, p, gx_send.at[v, k], gx_recv.at[v, k], over)

    def gather_0(v, t):
        for way in (1, -1):
            n = steps_of(STEPS_0, way)
            if t <= n:
                k = (-way * t) % NZ
                p = piece(v, side + at_z(k), 0)
                send_g0(v, way, t, p).wait_recv()
                if t < n:
                    go(send_g0(v, way, t + 1, p))
                go(send_gx(v, k, p))

    def gather_1(v, t):
        for jj in (1, 0):
            for way in (1, -1):
                n = steps_of(STEPS_1, way)
                if t <= n:
                    p = piece(v, x_of(jj) * NZ + at_z(-way * t), 1)
                    send_g1(v, jj, way, t, p).wait_recv()
                    if t < n:
                        go(send_g1(v, jj, way, t + 1, p))

    def end_a(v):
        xs[1, v, (1 - xl) * NZ + z] = last_1(v, 0).astype(BF16)
        go(cross(v))
        outer(v, 0, last_0(v))
        p = piece(v, me, 0)
        for way in (1, -1):
            go(send_g0(v, way, 1, p))
        go(send_gx(v, 0, p))

    def end_b(v):
        total_1 = last_1(v, 1)
        cross(v).wait_recv()
        outer(v, 1, total_1 + rx[v].astype(F32))
        p = piece(v, me, 1)
        go(send_gx(v, NZ, p))
        for way in (1, -1):
            go(send_g1(v, 1, way, 1, p))

    def end_c(v):
        p = piece(v, over, 1)
        send_gx(v, NZ, p).wait_recv()
        for way in (1, -1):
            go(send_g1(v, 0, way, 1, p))

    def both(step, *args):
        for v in range(WAVES):
            step(v, *args)

    both(first_0)
    for t in range(1, 4):
        both(reduce_step, t)
    for c in small:
        c.wait()
    both(end_a)
    end_b(0)
    both(gather_0, 1)
    for v in range(1, WAVES):
        end_b(v)
    end_c(0)
    both(gather_0, 2)
    for v in range(1, WAVES):
        end_c(v)
    both(gather_1, 1)
    both(gather_0, 3)
    both(gather_1, 2)
    both(gather_0, 4)
    both(gather_1, 3)
    both(gather_1, 4)
    for v in range(WAVES):
        for k in range(NZ):
            send_gx(v, k, piece(v, (1 - xl) * NZ + at_z(k), 0)).wait_recv()

    for c in sent:
        c.wait_send()
    send(a_out, a_in, ab_send.at[0], a_recv.at[0], pair).wait_send()

    @pl.when(jnp.logical_not(edge))
    def _():
        send(b_out, b_in, ab_send.at[1], b_recv.at[0], middle).wait_send()


def write_out(w_v, o_v, w_hbm, o_hbm, sem):
    copies = (
        pltpu.make_async_copy(w_v, w_hbm, sem.at[0]),
        pltpu.make_async_copy(o_v, o_hbm, sem.at[1]),
    )
    for c in copies:
        c.start()
    for c in copies:
        c.wait()


def per_device(weights, momentum, gradients, outer_momentum):
    rows, cols = weights.shape[1:]
    half, block = cols // 2, rows // (2 * NZ)
    part = block // WAVES
    chunks, groups = rows // CHUNK, rows // GROUP
    scale = 2 * 0.5 * 0.2 * math.sqrt(rows) / (2 * NZ)
    hbm_spec = pl.BlockSpec(memory_space=pltpu.HBM)
    any_spec = pl.BlockSpec(memory_space=pl.ANY)
    vmem_spec = pl.BlockSpec(memory_space=pltpu.VMEM)
    dma = pltpu.SemaphoreType.DMA
    new_weights, new_outer = pl.pallas_call(
        functools.partial(kernel, scale),
        out_shape=(pltpu.VMEM((rows, cols), BF16), pltpu.VMEM((block, cols), F32)),
        in_specs=[hbm_spec] * 4,
        out_specs=(vmem_spec, vmem_spec),
        scratch_shapes=[
            pltpu.VMEM((rows, cols), F32),
            pltpu.VMEM((2, rows, cols), BF16),
            pltpu.VMEM((block, cols), BF16),
            pltpu.VMEM((block, cols), F32),
            pltpu.VMEM((rows, cols), BF16),
            pltpu.VMEM((rows, cols), BF16),
            pltpu.VMEM((rows, cols), BF16),
            pltpu.VMEM((rows, cols), BF16),
            pltpu.VMEM((rows, cols), BF16),
            pltpu.VMEM((cols, cols), F32),
            pltpu.VMEM((cols, cols), F32),
            pltpu.VMEM((cols, cols), F32),
            pltpu.VMEM((8, cols), F32),
            pltpu.VMEM((cols, cols), BF16),
            pltpu.VMEM((2, WAVES, 2 * NZ, part, half), BF16),
            pltpu.VMEM((WAVES, NZ, part, half), BF16),
            pltpu.VMEM((WAVES, NZ - 1, part, half), BF16),
            pltpu.VMEM((WAVES, 2, NZ - 1, part, half), BF16),
            pltpu.VMEM((WAVES, part, half), BF16),
            dma((3, groups)),
            dma((2,)),
            dma((chunks,)), dma((chunks,)), dma((2,)),
            dma((WAVES, NZ)), dma((WAVES, NZ)),
            dma((WAVES, NZ - 1)), dma((WAVES, NZ - 1)),
            dma((WAVES, 2, NZ - 1)), dma((WAVES, 2, NZ - 1)),
            dma((WAVES,)), dma((WAVES,)),
            dma((WAVES, NZ - 1)), dma((WAVES, NZ - 1)),
            dma((WAVES, 2, NZ - 1)), dma((WAVES, 2, NZ - 1)),
            dma((WAVES, NZ + 1)), dma((WAVES, NZ + 1)),
        ],
        compiler_params=pltpu.CompilerParams(
            collective_id=0, has_side_effects=True, vmem_limit_bytes=48 * 1024 * 1024
        ),
        name="gossip_muon",
    )(*(
        pltpu.with_memory_space_constraint(a, pltpu.HBM)
        for a in (momentum[0, 0], gradients[:, 0, 0], weights[0], outer_momentum[0])
    ))
    new_weights, new_outer = pl.pallas_call(
        write_out,
        out_shape=(
            jax.ShapeDtypeStruct((rows, cols), BF16),
            jax.ShapeDtypeStruct((block, cols), F32),
        ),
        in_specs=[vmem_spec] * 2,
        out_specs=(any_spec, any_spec),
        scratch_shapes=[dma((2,))],
        name="write_out",
    )(
        pltpu.with_memory_space_constraint(new_weights, pltpu.VMEM),
        pltpu.with_memory_space_constraint(new_outer, pltpu.VMEM),
    )
    return new_weights[None], new_outer[None]


def solution(mesh):
    return jax.shard_map(
        per_device,
        mesh=mesh,
        in_specs=(
            P("expert", None, None),
            P("replica", "expert", None, None),
            P(None, "replica", "expert", None, None),
            P("expert", "replica", None),
        ),
        out_specs=(P("expert", None, None), P("expert", "replica", None)),
        check_vma=False,
    )
```

```python
import functools
import math

import jax
import jax.numpy as jnp
from jax import lax
from jax.experimental import pallas as pl
from jax.experimental.pallas import tpu as pltpu
from jax.sharding import PartitionSpec as P

A, B, C = 3.4445, -4.775, 2.0315
NZ = 8
MESH = pl.DeviceIdType.MESH
F32, BF16 = jnp.float32, jnp.bfloat16

CHUNK = 32
GROUP = 256
LAG = 4

STEPS_0 = ((4, 3), (3, 4))
STEPS_1 = ((3, 4), (4, 3))
PIECES = 4
WAVES = 2
ORDER = (
    ('first', 0), ('first', 1), ('reduce', 0, 1), ('reduce', 1, 1), ('reduce', 0, 2), ('reduce', 1, 2), ('reduce', 0, 3), ('reduce', 1, 3), ('a', 0), ('a', 1), ('b', 0), ('g0', 0, 1), ('g0', 1, 1), ('b', 1), ('c', 0), ('g0', 0, 2), ('g0', 1, 2), ('c', 1), ('g1', 0, 1), ('g1', 1, 1), ('g0', 0, 3), ('g0', 1, 3), ('g1', 0, 2), ('g1', 1, 2), ('g0', 0, 4), ('g0', 1, 4), ('g1', 0, 3), ('g1', 1, 3), ('g1', 0, 4), ('g1', 1, 4),
)
X_ORDER = (4, 5, 3, 6, 2, 7, 1, 0)


def dot(a, b):
    return jnp.dot(a, b, preferred_element_type=F32)


def dot_t(a, b):
    return lax.dot_general(a, b, (((0,), (0,)), ((), ())), preferred_element_type=F32)


def kernel(
    scale, m_hbm, g_hbm, w_hbm, o_hbm, out_v, no_v,
    m_v, g_v, w_v, o_v,
    a_in, b_in, a_out, b_out, x0, gram, d0, f_v, norm, e_v, xs, xr, r0, r1, rx,
    load_sem, small_sem,
    a_recv, b_recv, ab_send, send_sem,
    xr_recv, r0_recv, r1_recv, rx_recv, g0_recv, g1_recv, gx_recv,
):
    rows, cols = m_v.shape
    half = cols // 2
    block = rows // (2 * NZ)
    part = block // WAVES
    chunks, groups, per = rows // CHUNK, rows // GROUP, GROUP // CHUNK
    me = lax.axis_index("replica")
    xl, z = me // NZ, lax.rem(me, NZ)
    over = (1 - xl) * NZ + z
    side = xl * NZ

    def at_z(offset):
        return lax.rem(z + offset + NZ, NZ)

    up, down = side + at_z(1), side + at_z(-1)
    q = lax.rem(z, 4)
    edge = jnp.logical_or(q == 0, q == 3)
    pair = side + z + 1 - 2 * lax.rem(z, 2)
    middle = side + lax.rem(jnp.where(q == 1, z + 1, z + NZ - 1), NZ)

    def send(src, dst, send_sem, recv_sem, to):
        return pltpu.make_async_remote_copy(
            src_ref=src, dst_ref=dst, send_sem=send_sem, recv_sem=recv_sem,
            device_id={"replica": to}, device_id_type=MESH,
        )

    def span(i, n):
        return pl.ds(pl.multiple_of(i * n, n), n)

    def start_load(i):
        s = span(i, GROUP)
        pltpu.make_async_copy(m_hbm.at[s], m_v.at[s], load_sem.at[i]).start()
        pltpu.make_async_copy(g_hbm.at[:, s], g_v.at[:, s], load_sem.at[i]).start()

    def wait_load(i):
        s = pl.ds(0, 2 * GROUP)
        pltpu.make_async_copy(m_hbm.at[s], m_v.at[s], load_sem.at[i]).wait()

    for i in range(groups):
        start_load(i)
    own_rows = span(me, block)
    small = (
        pltpu.make_async_copy(w_hbm.at[own_rows], w_v, small_sem.at[0]),
        pltpu.make_async_copy(o_hbm, o_v, small_sem.at[1]),
    )
    for c in small:
        c.start()

    barrier = pltpu.get_barrier_semaphore()
    for other in (up, down, over):
        pl.semaphore_signal(barrier, inc=1, device_id={"replica": other}, device_id_type=MESH)
    pl.semaphore_wait(barrier, 3)

    gram[...] = jnp.zeros_like(gram)
    norm[...] = jnp.zeros_like(norm)

    def moment(s):
        return 0.9 * m_v[s, :] + g_v[0, s, :].astype(F32)

    def send_a(i):
        s = span(i, CHUNK)
        return send(a_out.at[s], a_in.at[s], ab_send.at[0], a_recv.at[i], pair)

    def send_b(i):
        s = span(i, CHUNK)
        return send(b_out.at[s], b_in.at[s], ab_send.at[1], b_recv.at[i], middle)

    def keep(s, value):
        x0[s, :] = value.astype(BF16)
        squares = (value * value).reshape(CHUNK // 8, 8, cols)
        norm[...] += jnp.sum(squares, axis=0)

    def add_gram(j):
        x = x0[span(j, GROUP), :]
        gram[...] += dot_t(x, x)

    @pl.when(edge)
    def _():
        @pl.loop(0, groups)
        def _(j):
            wait_load(j)
            for k in range(per):
                i = j * per + k
                s = span(i, CHUNK)
                a_out[s, :] = moment(s).astype(BF16)
                send_a(i).start()

        @pl.loop(0, groups)
        def _(j):
            for k in range(per):
                i = j * per + k
                s = span(i, CHUNK)
                send_a(i).wait_recv()
                keep(s, a_in[s, :].astype(F32) + 0.225 * moment(s) + 0.5 * g_v[1, s, :].astype(F32))
            add_gram(j)

    @pl.when(jnp.logical_not(edge))
    def _():
        def second(i):
            s = span(i, CHUNK)
            send_b(i).wait_recv()
            a_out[s, :] = (b_in[s, :].astype(F32) + 0.225 * moment(s)).astype(BF16)
            send_a(i).start()

        @pl.loop(0, groups)
        def _(j):
            wait_load(j)
            for k in range(per):
                i = j * per + k
                s = span(i, CHUNK)
                send_a(i).wait_recv()
                mean = 0.5 * (a_in[s, :].astype(F32) + moment(s))
                b_out[s, :] = (0.45 * mean + 0.5 * g_v[1, s, :].astype(F32)).astype(BF16)
                send_b(i).start()
                keep(s, mean)
                if k >= LAG:
                    second(i - LAG)
                else:
                    pl.when(j > 0)(functools.partial(second, i - LAG))
            add_gram(j)

        for i in range(chunks - LAG, chunks):
            second(i)

    total = jnp.sum(jnp.sum(norm[...], axis=0, keepdims=True), axis=1, keepdims=True)
    unit = 1.0 / (jnp.sqrt(total) + 1e-7)

    g = gram[...] * (unit * unit)
    gh = g.astype(BF16)
    d = B * g + C * dot(gh, gh)
    d0[...] = d
    dh = d.astype(BF16)
    t = dot(gh, dh)
    gram[...] = (A * A) * g + (2 * A) * t + dot(t.astype(BF16), dh)

    g = gram[...]
    gh = g.astype(BF16)
    d = B * g + C * dot(gh, gh)
    dh = d.astype(BF16)
    first = d0[...]
    f_v[...] = A * (first + d) + dot(first.astype(BF16), dh)
    t = dot(gh, dh)
    gram[...] = (A * A) * g + (2 * A) * t + dot(t.astype(BF16), dh)

    g = gram[...]
    gh = g.astype(BF16)
    d = B * g + C * dot(gh, gh)
    f = f_v[...]
    e = (A * A) * d + A * f + dot(f.astype(BF16), d.astype(BF16))
    factor = unit * scale
    e_v[...] = (e * factor).astype(BF16)
    lead = factor * (A * A * A)

    def send_xr(v, k):
        zz = at_z(k)
        src = xs.at[0, v, (1 - xl) * NZ + zz]
        return send(src, xr.at[v, zz], send_sem.at[0], xr_recv.at[v, k], over)

    def slot(steps, way, t):
        return (0 if way > 0 else steps[0]) + t - 1

    def steps_of(steps, way):
        return steps[0] if way > 0 else steps[1]

    def towards(way):
        return up if way > 0 else down

    def x_of(jj):
        return 1 - xl if jj == 0 else xl

    def send_r0(v, way, t, src):
        i = slot(STEPS_0[v], way, t)
        return send(src, r0.at[v, i], send_sem.at[0], r0_recv.at[v, i], towards(way))

    def send_r1(v, jj, way, t, src):
        i = slot(STEPS_1[v], way, t)
        return send(src, r1.at[v, jj, i], send_sem.at[0], r1_recv.at[v, jj, i], towards(way))

    def offset(way, n, t):
        return way * (n + 1 - t)

    sent = [0, 0]

    def go(c, phase=0):
        sent[phase] += part // 2
        c.start()

    e = e_v[...]
    for k in X_ORDER:
        zz = at_z(k)
        x = jnp.concatenate([x0[span(zz, block), :], x0[span(NZ + zz, block), :]], axis=0)
        y = (lead * x.astype(F32) + dot(x, e)).astype(BF16)
        for v in range(WAVES):
            for h in range(2):
                c = slice(h * half, (h + 1) * half)
                xs[h, v, zz] = y[v * part : (v + 1) * part, c]
                xs[h, v, NZ + zz] = y[block + v * part : block + (v + 1) * part, c]
        for v in range(WAVES):
            go(send_xr(v, k))
            for way in (1, -1):
                n = steps_of(STEPS_1[v], way)
                if (way * n) % NZ == k:
                    for jj in range(2):
                        go(send_r1(v, jj, way, 1, xs.at[1, v, x_of(jj) * NZ + zz]))

    def own_0(v, k):
        send_xr(v, k % NZ).wait_recv()
        zz = at_z(k)
        return zz, xs[0, v, side + zz].astype(F32) + xr[v, zz].astype(F32)

    def first_0(v):
        for way in (1, -1):
            zz, own = own_0(v, offset(way, steps_of(STEPS_0[v], way), 1))
            xr[v, zz] = own.astype(BF16)
            go(send_r0(v, way, 1, xr.at[v, zz]))

    def forward_0(v, way, t):
        n = steps_of(STEPS_0[v], way)
        i = slot(STEPS_0[v], way, t)
        send_r0(v, way, t, r0.at[v, i]).wait_recv()
        _, own = own_0(v, offset(way, n, t + 1))
        r0[v, i] = (r0[v, i].astype(F32) + own).astype(BF16)
        go(send_r0(v, way, t + 1, r0.at[v, i]))

    def forward_1(v, jj, way, t):
        n = steps_of(STEPS_1[v], way)
        i = slot(STEPS_1[v], way, t)
        send_r1(v, jj, way, t, r1.at[v, jj, i]).wait_recv()
        own = xs[1, v, x_of(jj) * NZ + at_z(offset(way, n, t + 1))]
        r1[v, jj, i] = (r1[v, jj, i].astype(F32) + own.astype(F32)).astype(BF16)
        go(send_r1(v, jj, way, t + 1, r1.at[v, jj, i]))

    def reduce_step(v, t):
        for jj in range(2):
            for way in (1, -1):
                if t < steps_of(STEPS_1[v], way):
                    forward_1(v, jj, way, t)
        for way in (1, -1):
            if t < steps_of(STEPS_0[v], way):
                forward_0(v, way, t)

    def last_1(v, jj):
        out = xs[1, v, x_of(jj) * NZ + z].astype(F32)
        for way in (1, -1):
            n = steps_of(STEPS_1[v], way)
            i = slot(STEPS_1[v], way, n)
            send_r1(v, jj, way, n, r1.at[v, jj, i]).wait_recv()
            out += r1[v, jj, i].astype(F32)
        return out

    def last_0(v):
        _, out = own_0(v, 0)
        for way in (1, -1):
            n = steps_of(STEPS_0[v], way)
            i = slot(STEPS_0[v], way, n)
            send_r0(v, way, n, r0.at[v, i]).wait_recv()
            out += r0[v, i].astype(F32)
        return out

    def cross(v):
        src = xs.at[1, v, (1 - xl) * NZ + z]
        return send(src, rx.at[v], send_sem.at[0], rx_recv.at[v], over)

    def rows_of(v, b):
        return pl.ds(pl.multiple_of(b * block + v * part, part), part)

    def piece(v, b, h):
        return out_v.at[rows_of(v, b), pl.ds(h * half, half)]

    def outer(v, h, delta):
        r, c = slice(v * part, (v + 1) * part), slice(h * half, (h + 1) * half)
        fresh = 0.9 * o_v[r, c] + delta
        no_v[r, c] = fresh
        out_v[rows_of(v, me), c] = (w_v[r, c].astype(F32) - fresh).astype(BF16)

    def send_g0(v, way, t, p):
        i = slot(STEPS_0[v], way, t)
        return send(p, p, send_sem.at[1], g0_recv.at[v, i], towards(way))

    def send_g1(v, jj, way, t, p):
        i = slot(STEPS_1[v], way, t)
        return send(p, p, send_sem.at[1], g1_recv.at[v, jj, i], towards(way))

    def send_gx(v, k, p):
        return send(p, p, send_sem.at[1], gx_recv.at[v, k], over)

    def gather_0(v, t):
        for way in (1, -1):
            n = steps_of(STEPS_0[v], way)
            if t <= n:
                k = (-way * t) % NZ
                p = piece(v, side + at_z(k), 0)
                send_g0(v, way, t, p).wait_recv()
                if t < n:
                    go(send_g0(v, way, t + 1, p), 1)
                go(send_gx(v, k, p), 1)

    def gather_1(v, t):
        for jj in (1, 0):
            for way in (1, -1):
                n = steps_of(STEPS_1[v], way)
                if t <= n:
                    p = piece(v, x_of(jj) * NZ + at_z(-way * t), 1)
                    send_g1(v, jj, way, t, p).wait_recv()
                    if t < n:
                        go(send_g1(v, jj, way, t + 1, p), 1)

    def end_a(v):
        xs[1, v, (1 - xl) * NZ + z] = last_1(v, 0).astype(BF16)
        go(cross(v))
        outer(v, 0, last_0(v))
        p = piece(v, me, 0)
        for way in (1, -1):
            go(send_g0(v, way, 1, p), 1)
        go(send_gx(v, 0, p), 1)

    def end_b(v):
        total_1 = last_1(v, 1)
        cross(v).wait_recv()
        outer(v, 1, total_1 + rx[v].astype(F32))
        p = piece(v, me, 1)
        go(send_gx(v, NZ, p), 1)
        for way in (1, -1):
            go(send_g1(v, 1, way, 1, p), 1)

    def end_c(v):
        p = piece(v, over, 1)
        send_gx(v, NZ, p).wait_recv()
        for way in (1, -1):
            go(send_g1(v, 0, way, 1, p), 1)

    steps = dict(
        first=first_0, reduce=reduce_step, a=end_a, b=end_b, c=end_c, g0=gather_0, g1=gather_1
    )
    for c in small:
        c.wait()
    for step, *args in ORDER:
        steps[step](*args)
    for v in range(WAVES):
        for k in range(NZ):
            send_gx(v, k, piece(v, (1 - xl) * NZ + at_z(k), 0)).wait_recv()

    for phase in range(2):
        r = pl.ds(0, sent[phase])
        send(a_out.at[r], a_in.at[r], send_sem.at[phase], a_recv.at[0], pair).wait_send()
    send(a_out, a_in, ab_send.at[0], a_recv.at[0], pair).wait_send()

    @pl.when(jnp.logical_not(edge))
    def _():
        send(b_out, b_in, ab_send.at[1], b_recv.at[0], middle).wait_send()


def write_out(w_v, o_v, w_hbm, o_hbm, sem):
    n = w_v.shape[0] // PIECES
    copies = [pltpu.make_async_copy(o_v, o_hbm, sem.at[PIECES])]
    for i in range(PIECES):
        s = pl.ds(i * n, n)
        copies.append(pltpu.make_async_copy(w_v.at[s], w_hbm.at[s], sem.at[i]))
    for c in copies:
        c.start()
    for c in copies:
        c.wait()


def per_device(weights, momentum, gradients, outer_momentum):
    rows, cols = weights.shape[1:]
    half, block = cols // 2, rows // (2 * NZ)
    part = block // WAVES
    chunks, groups = rows // CHUNK, rows // GROUP
    scale = 2 * 0.5 * 0.2 * math.sqrt(rows) / (2 * NZ)
    hbm_spec = pl.BlockSpec(memory_space=pltpu.HBM)
    any_spec = pl.BlockSpec(memory_space=pl.ANY)
    vmem_spec = pl.BlockSpec(memory_space=pltpu.VMEM)
    dma = pltpu.SemaphoreType.DMA
    new_weights, new_outer = pl.pallas_call(
        functools.partial(kernel, scale),
        out_shape=(pltpu.VMEM((rows, cols), BF16), pltpu.VMEM((block, cols), F32)),
        in_specs=[hbm_spec] * 4,
        out_specs=(vmem_spec, vmem_spec),
        scratch_shapes=[
            pltpu.VMEM((rows, cols), F32),
            pltpu.VMEM((2, rows, cols), BF16),
            pltpu.VMEM((block, cols), BF16),
            pltpu.VMEM((block, cols), F32),
            pltpu.VMEM((rows, cols), BF16),
            pltpu.VMEM((rows, cols), BF16),
            pltpu.VMEM((rows, cols), BF16),
            pltpu.VMEM((rows, cols), BF16),
            pltpu.VMEM((rows, cols), BF16),
            pltpu.VMEM((cols, cols), F32),
            pltpu.VMEM((cols, cols), F32),
            pltpu.VMEM((cols, cols), F32),
            pltpu.VMEM((8, cols), F32),
            pltpu.VMEM((cols, cols), BF16),
            pltpu.VMEM((2, WAVES, 2 * NZ, part, half), BF16),
            pltpu.VMEM((WAVES, NZ, part, half), BF16),
            pltpu.VMEM((WAVES, NZ - 1, part, half), BF16),
            pltpu.VMEM((WAVES, 2, NZ - 1, part, half), BF16),
            pltpu.VMEM((WAVES, part, half), BF16),
            dma((groups,)),
            dma((2,)),
            dma((chunks,)), dma((chunks,)), dma((2,)),
            dma((2,)),
            dma((WAVES, NZ)),
            dma((WAVES, NZ - 1)),
            dma((WAVES, 2, NZ - 1)),
            dma((WAVES,)),
            dma((WAVES, NZ - 1)),
            dma((WAVES, 2, NZ - 1)),
            dma((WAVES, NZ + 1)),
        ],
        compiler_params=pltpu.CompilerParams(
            collective_id=0, has_side_effects=True, vmem_limit_bytes=48 * 1024 * 1024
        ),
        name="gossip_muon",
    )(*(
        pltpu.with_memory_space_constraint(a, pltpu.HBM)
        for a in (momentum[0, 0], gradients[:, 0, 0], weights[0], outer_momentum[0])
    ))
    new_weights, new_outer = pl.pallas_call(
        write_out,
        out_shape=(
            jax.ShapeDtypeStruct((rows, cols), BF16),
            jax.ShapeDtypeStruct((block, cols), F32),
        ),
        in_specs=[vmem_spec] * 2,
        out_specs=(any_spec, any_spec),
        scratch_shapes=[dma((PIECES + 1,))],
        name="write_out",
    )(
        pltpu.with_memory_space_constraint(new_weights, pltpu.VMEM),
        pltpu.with_memory_space_constraint(new_outer, pltpu.VMEM),
    )
    return new_weights[None], new_outer[None]


def solution(mesh):
    return jax.shard_map(
        per_device,
        mesh=mesh,
        in_specs=(
            P("expert", None, None),
            P("replica", "expert", None, None),
            P(None, "replica", "expert", None, None),
            P("expert", "replica", None),
        ),
        out_specs=(P("expert", None, None), P("expert", "replica", None)),
        check_vma=False,
    )
```

```python
import functools
import math

import jax
import jax.numpy as jnp
from jax import lax
from jax.experimental import pallas as pl
from jax.experimental.pallas import tpu as pltpu
from jax.sharding import PartitionSpec as P

A, B, C = 3.4445, -4.775, 2.0315
NZ = 8
MESH = pl.DeviceIdType.MESH
F32, BF16 = jnp.float32, jnp.bfloat16

CHUNK = 32
GROUP = 128
LAG = 4

STEPS_0 = ((4, 3), (4, 3))
STEPS_1 = ((3, 4), (3, 4))
PIECES = 4
WAVES = 2
ORDER = (
    ('first', 0), ('first', 1), ('reduce', 0, 1), ('reduce', 1, 1), ('reduce', 0, 2), ('reduce', 1, 2), ('reduce', 0, 3), ('reduce', 1, 3), ('a', 0), ('a', 1), ('b', 0), ('g0', 0, 1), ('g0', 1, 1), ('b', 1), ('c', 0), ('g0', 0, 2), ('g0', 1, 2), ('c', 1), ('g1', 0, 1), ('g1', 1, 1), ('g0', 0, 3), ('g0', 1, 3), ('g1', 0, 2), ('g1', 1, 2), ('g0', 0, 4), ('g0', 1, 4), ('g1', 0, 3), ('g1', 1, 3), ('g1', 0, 4), ('g1', 1, 4),
)
X_ORDER = (4, 5, 3, 6, 2, 7, 1, 0)


def dot(a, b):
    return jnp.dot(a, b, preferred_element_type=F32)


def dot_t(a, b):
    return lax.dot_general(a, b, (((0,), (0,)), ((), ())), preferred_element_type=F32)


def kernel(
    scale, m_hbm, g_hbm, w_hbm, o_hbm, out_v, no_v,
    m_v, g_v, w_v, o_v,
    a_in, b_in, a_out, b_out, x0, gram, d0, f_v, norm, e_v, xs, xr, r0, r1, rx,
    load_sem, small_sem,
    a_recv, b_recv, ab_send, send_sem,
    xr_recv, r0_recv, r1_recv, rx_recv, g0_recv, g1_recv, gx_recv,
):
    rows, cols = m_v.shape
    half = cols // 2
    block = rows // (2 * NZ)
    part = block // WAVES
    chunks, groups, per = rows // CHUNK, rows // GROUP, GROUP // CHUNK
    me = lax.axis_index("replica")
    xl, z = me // NZ, lax.rem(me, NZ)
    over = (1 - xl) * NZ + z
    side = xl * NZ

    def at_z(offset):
        return lax.rem(z + offset + NZ, NZ)

    up, down = side + at_z(1), side + at_z(-1)
    q = lax.rem(z, 4)
    edge = jnp.logical_or(q == 0, q == 3)
    pair = side + z + 1 - 2 * lax.rem(z, 2)
    middle = side + lax.rem(jnp.where(q == 1, z + 1, z + NZ - 1), NZ)

    def send(src, dst, send_sem, recv_sem, to):
        return pltpu.make_async_remote_copy(
            src_ref=src, dst_ref=dst, send_sem=send_sem, recv_sem=recv_sem,
            device_id={"replica": to}, device_id_type=MESH,
        )

    def span(i, n):
        return pl.ds(pl.multiple_of(i * n, n), n)

    def start_load(i):
        s = span(i, GROUP)
        pltpu.make_async_copy(m_hbm.at[s], m_v.at[s], load_sem.at[i]).start()
        pltpu.make_async_copy(g_hbm.at[:, s], g_v.at[:, s], load_sem.at[i]).start()

    def wait_load(i):
        s = pl.ds(0, 2 * GROUP)
        pltpu.make_async_copy(m_hbm.at[s], m_v.at[s], load_sem.at[i]).wait()

    for i in range(groups):
        start_load(i)
    own_rows = span(me, block)
    small = (
        pltpu.make_async_copy(w_hbm.at[own_rows], w_v, small_sem.at[0]),
        pltpu.make_async_copy(o_hbm, o_v, small_sem.at[1]),
    )
    for c in small:
        c.start()

    barrier = pltpu.get_barrier_semaphore()
    for other in (up, down, over):
        pl.semaphore_signal(barrier, inc=1, device_id={"replica": other}, device_id_type=MESH)
    pl.semaphore_wait(barrier, 3)

    gram[...] = jnp.zeros_like(gram)
    norm[...] = jnp.zeros_like(norm)

    def moment(s):
        return 0.9 * m_v[s, :] + g_v[0, s, :].astype(F32)

    def send_a(i):
        s = span(i, CHUNK)
        return send(a_out.at[s], a_in.at[s], ab_send.at[0], a_recv.at[i], pair)

    def send_b(i):
        s = span(i, CHUNK)
        return send(b_out.at[s], b_in.at[s], ab_send.at[1], b_recv.at[i], middle)

    def keep(s, value):
        x0[s, :] = value.astype(BF16)
        squares = (value * value).reshape(CHUNK // 8, 8, cols)
        norm[...] += jnp.sum(squares, axis=0)

    def add_gram(j):
        x = x0[span(j, GROUP), :]
        gram[...] += dot_t(x, x)

    @pl.when(edge)
    def _():
        @pl.loop(0, groups)
        def _(j):
            wait_load(j)
            for k in range(per):
                i = j * per + k
                s = span(i, CHUNK)
                a_out[s, :] = moment(s).astype(BF16)
                send_a(i).start()

        @pl.loop(0, groups)
        def _(j):
            for k in range(per):
                i = j * per + k
                s = span(i, CHUNK)
                send_a(i).wait_recv()
                keep(s, a_in[s, :].astype(F32) + 0.225 * moment(s) + 0.5 * g_v[1, s, :].astype(F32))
            add_gram(j)

    @pl.when(jnp.logical_not(edge))
    def _():
        def second(i):
            s = span(i, CHUNK)
            send_b(i).wait_recv()
            a_out[s, :] = (b_in[s, :].astype(F32) + 0.225 * moment(s)).astype(BF16)
            send_a(i).start()

        @pl.loop(0, groups)
        def _(j):
            wait_load(j)
            for k in range(per):
                i = j * per + k
                s = span(i, CHUNK)
                send_a(i).wait_recv()
                mean = 0.5 * (a_in[s, :].astype(F32) + moment(s))
                b_out[s, :] = (0.45 * mean + 0.5 * g_v[1, s, :].astype(F32)).astype(BF16)
                send_b(i).start()
                keep(s, mean)
                if k >= LAG:
                    second(i - LAG)
                else:
                    pl.when(j > 0)(functools.partial(second, i - LAG))
            add_gram(j)

        for i in range(chunks - LAG, chunks):
            second(i)

    total = jnp.sum(jnp.sum(norm[...], axis=0, keepdims=True), axis=1, keepdims=True)
    unit = 1.0 / (jnp.sqrt(total) + 1e-7)

    g = gram[...] * (unit * unit)
    gh = g.astype(BF16)
    d = B * g + C * dot(gh, gh)
    d0[...] = d
    dh = d.astype(BF16)
    t = dot(gh, dh)
    gram[...] = (A * A) * g + (2 * A) * t + dot(t.astype(BF16), dh)

    g = gram[...]
    gh = g.astype(BF16)
    d = B * g + C * dot(gh, gh)
    dh = d.astype(BF16)
    first = d0[...]
    f_v[...] = A * (first + d) + dot(first.astype(BF16), dh)
    t = dot(gh, dh)
    gram[...] = (A * A) * g + (2 * A) * t + dot(t.astype(BF16), dh)

    g = gram[...]
    gh = g.astype(BF16)
    d = B * g + C * dot(gh, gh)
    f = f_v[...]
    e = (A * A) * d + A * f + dot(f.astype(BF16), d.astype(BF16))
    factor = unit * scale
    e_v[...] = (e * factor).astype(BF16)
    lead = factor * (A * A * A)

    def send_xr(v, k):
        zz = at_z(k)
        src = xs.at[0, v, (1 - xl) * NZ + zz]
        return send(src, xr.at[v, zz], send_sem.at[0], xr_recv.at[v, k], over)

    def slot(steps, way, t):
        return (0 if way > 0 else steps[0]) + t - 1

    def steps_of(steps, way):
        return steps[0] if way > 0 else steps[1]

    def towards(way):
        return up if way > 0 else down

    def x_of(jj):
        return 1 - xl if jj == 0 else xl

    def send_r0(v, way, t, src):
        i = slot(STEPS_0[v], way, t)
        return send(src, r0.at[v, i], send_sem.at[0], r0_recv.at[v, i], towards(way))

    def send_r1(v, jj, way, t, src):
        i = slot(STEPS_1[v], way, t)
        return send(src, r1.at[v, jj, i], send_sem.at[0], r1_recv.at[v, jj, i], towards(way))

    def offset(way, n, t):
        return way * (n + 1 - t)

    sent = [0, 0]

    def go(c, phase=0):
        sent[phase] += part // 2
        c.start()

    e = e_v[...]
    for k in X_ORDER:
        zz = at_z(k)
        x = jnp.concatenate([x0[span(zz, block), :], x0[span(NZ + zz, block), :]], axis=0)
        y = (lead * x.astype(F32) + dot(x, e)).astype(BF16)
        for v in range(WAVES):
            for h in range(2):
                c = slice(h * half, (h + 1) * half)
                xs[h, v, zz] = y[v * part : (v + 1) * part, c]
                xs[h, v, NZ + zz] = y[block + v * part : block + (v + 1) * part, c]
        for v in range(WAVES):
            go(send_xr(v, k))
            for way in (1, -1):
                n = steps_of(STEPS_1[v], way)
                if (way * n) % NZ == k:
                    for jj in range(2):
                        go(send_r1(v, jj, way, 1, xs.at[1, v, x_of(jj) * NZ + zz]))

    def own_0(v, k):
        send_xr(v, k % NZ).wait_recv()
        zz = at_z(k)
        return zz, xs[0, v, side + zz].astype(F32) + xr[v, zz].astype(F32)

    def first_0(v):
        for way in (1, -1):
            zz, own = own_0(v, offset(way, steps_of(STEPS_0[v], way), 1))
            xr[v, zz] = own.astype(BF16)
            go(send_r0(v, way, 1, xr.at[v, zz]))

    def forward_0(v, way, t):
        n = steps_of(STEPS_0[v], way)
        i = slot(STEPS_0[v], way, t)
        send_r0(v, way, t, r0.at[v, i]).wait_recv()
        _, own = own_0(v, offset(way, n, t + 1))
        r0[v, i] = (r0[v, i].astype(F32) + own).astype(BF16)
        go(send_r0(v, way, t + 1, r0.at[v, i]))

    def forward_1(v, jj, way, t):
        n = steps_of(STEPS_1[v], way)
        i = slot(STEPS_1[v], way, t)
        send_r1(v, jj, way, t, r1.at[v, jj, i]).wait_recv()
        own = xs[1, v, x_of(jj) * NZ + at_z(offset(way, n, t + 1))]
        r1[v, jj, i] = (r1[v, jj, i].astype(F32) + own.astype(F32)).astype(BF16)
        go(send_r1(v, jj, way, t + 1, r1.at[v, jj, i]))

    def reduce_step(v, t):
        for jj in range(2):
            for way in (1, -1):
                if t < steps_of(STEPS_1[v], way):
                    forward_1(v, jj, way, t)
        for way in (1, -1):
            if t < steps_of(STEPS_0[v], way):
                forward_0(v, way, t)

    def last_1(v, jj):
        out = xs[1, v, x_of(jj) * NZ + z].astype(F32)
        for way in (1, -1):
            n = steps_of(STEPS_1[v], way)
            i = slot(STEPS_1[v], way, n)
            send_r1(v, jj, way, n, r1.at[v, jj, i]).wait_recv()
            out += r1[v, jj, i].astype(F32)
        return out

    def last_0(v):
        _, out = own_0(v, 0)
        for way in (1, -1):
            n = steps_of(STEPS_0[v], way)
            i = slot(STEPS_0[v], way, n)
            send_r0(v, way, n, r0.at[v, i]).wait_recv()
            out += r0[v, i].astype(F32)
        return out

    def cross(v):
        src = xs.at[1, v, (1 - xl) * NZ + z]
        return send(src, rx.at[v], send_sem.at[0], rx_recv.at[v], over)

    def rows_of(v, b):
        return pl.ds(pl.multiple_of(b * block + v * part, part), part)

    def piece(v, b, h):
        return out_v.at[rows_of(v, b), pl.ds(h * half, half)]

    def outer(v, h, delta):
        r, c = slice(v * part, (v + 1) * part), slice(h * half, (h + 1) * half)
        fresh = 0.9 * o_v[r, c] + delta
        no_v[r, c] = fresh
        out_v[rows_of(v, me), c] = (w_v[r, c].astype(F32) - fresh).astype(BF16)

    def send_g0(v, way, t, p):
        i = slot(STEPS_0[v], way, t)
        return send(p, p, send_sem.at[1], g0_recv.at[v, i], towards(way))

    def send_g1(v, jj, way, t, p):
        i = slot(STEPS_1[v], way, t)
        return send(p, p, send_sem.at[1], g1_recv.at[v, jj, i], towards(way))

    def send_gx(v, k, p):
        return send(p, p, send_sem.at[1], gx_recv.at[v, k // NZ], over)

    def gather_0(v, t):
        for way in (1, -1):
            n = steps_of(STEPS_0[v], way)
            if t <= n:
                k = (-way * t) % NZ
                p = piece(v, side + at_z(k), 0)
                send_g0(v, way, t, p).wait_recv()
                if t < n:
                    go(send_g0(v, way, t + 1, p), 1)
                go(send_gx(v, k, p), 1)

    def gather_1(v, t):
        for jj in (1, 0):
            for way in (1, -1):
                n = steps_of(STEPS_1[v], way)
                if t <= n:
                    p = piece(v, x_of(jj) * NZ + at_z(-way * t), 1)
                    send_g1(v, jj, way, t, p).wait_recv()
                    if t < n:
                        go(send_g1(v, jj, way, t + 1, p), 1)

    def end_a(v):
        xs[1, v, (1 - xl) * NZ + z] = last_1(v, 0).astype(BF16)
        go(cross(v))
        outer(v, 0, last_0(v))
        p = piece(v, me, 0)
        for way in (1, -1):
            go(send_g0(v, way, 1, p), 1)
        go(send_gx(v, 0, p), 1)

    def end_b(v):
        total_1 = last_1(v, 1)
        cross(v).wait_recv()
        outer(v, 1, total_1 + rx[v].astype(F32))
        p = piece(v, me, 1)
        go(send_gx(v, NZ, p), 1)
        for way in (1, -1):
            go(send_g1(v, 1, way, 1, p), 1)

    def end_c(v):
        p = piece(v, over, 1)
        send_gx(v, NZ, p).wait_recv()
        for way in (1, -1):
            go(send_g1(v, 0, way, 1, p), 1)

    steps = dict(
        first=first_0, reduce=reduce_step, a=end_a, b=end_b, c=end_c, g0=gather_0, g1=gather_1
    )
    for c in small:
        c.wait()
    for step, *args in ORDER:
        steps[step](*args)
    for v in range(WAVES):
        r = pl.ds(0, NZ * part // 2)
        send(a_out.at[r], a_in.at[r], send_sem.at[1], gx_recv.at[v, 0], over).wait_recv()

    for phase in range(2):
        r = pl.ds(0, sent[phase])
        send(a_out.at[r], a_in.at[r], send_sem.at[phase], a_recv.at[0], pair).wait_send()
    send(a_out, a_in, ab_send.at[0], a_recv.at[0], pair).wait_send()

    @pl.when(jnp.logical_not(edge))
    def _():
        send(b_out, b_in, ab_send.at[1], b_recv.at[0], middle).wait_send()


def write_out(w_v, o_v, w_hbm, o_hbm, sem):
    n = w_v.shape[0] // PIECES
    copies = [pltpu.make_async_copy(o_v, o_hbm, sem.at[PIECES])]
    for i in range(PIECES):
        s = pl.ds(i * n, n)
        copies.append(pltpu.make_async_copy(w_v.at[s], w_hbm.at[s], sem.at[i]))
    for c in copies:
        c.start()
    for c in copies:
        c.wait()


def per_device(weights, momentum, gradients, outer_momentum):
    rows, cols = weights.shape[1:]
    half, block = cols // 2, rows // (2 * NZ)
    part = block // WAVES
    chunks, groups = rows // CHUNK, rows // GROUP
    scale = 2 * 0.5 * 0.2 * math.sqrt(rows) / (2 * NZ)
    hbm_spec = pl.BlockSpec(memory_space=pltpu.HBM)
    any_spec = pl.BlockSpec(memory_space=pl.ANY)
    vmem_spec = pl.BlockSpec(memory_space=pltpu.VMEM)
    dma = pltpu.SemaphoreType.DMA
    new_weights, new_outer = pl.pallas_call(
        functools.partial(kernel, scale),
        out_shape=(pltpu.VMEM((rows, cols), BF16), pltpu.VMEM((block, cols), F32)),
        in_specs=[hbm_spec] * 4,
        out_specs=(vmem_spec, vmem_spec),
        scratch_shapes=[
            pltpu.VMEM((rows, cols), F32),
            pltpu.VMEM((2, rows, cols), BF16),
            pltpu.VMEM((block, cols), BF16),
            pltpu.VMEM((block, cols), F32),
            pltpu.VMEM((rows, cols), BF16),
            pltpu.VMEM((rows, cols), BF16),
            pltpu.VMEM((rows, cols), BF16),
            pltpu.VMEM((rows, cols), BF16),
            pltpu.VMEM((rows, cols), BF16),
            pltpu.VMEM((cols, cols), F32),
            pltpu.VMEM((cols, cols), F32),
            pltpu.VMEM((cols, cols), F32),
            pltpu.VMEM((8, cols), F32),
            pltpu.VMEM((cols, cols), BF16),
            pltpu.VMEM((2, WAVES, 2 * NZ, part, half), BF16),
            pltpu.VMEM((WAVES, NZ, part, half), BF16),
            pltpu.VMEM((WAVES, NZ - 1, part, half), BF16),
            pltpu.VMEM((WAVES, 2, NZ - 1, part, half), BF16),
            pltpu.VMEM((WAVES, part, half), BF16),
            dma((groups,)),
            dma((2,)),
            dma((chunks,)), dma((chunks,)), dma((2,)),
            dma((2,)),
            dma((WAVES, NZ)),
            dma((WAVES, NZ - 1)),
            dma((WAVES, 2, NZ - 1)),
            dma((WAVES,)),
            dma((WAVES, NZ - 1)),
            dma((WAVES, 2, NZ - 1)),
            dma((WAVES, 2)),
        ],
        compiler_params=pltpu.CompilerParams(
            collective_id=0, has_side_effects=True, vmem_limit_bytes=48 * 1024 * 1024
        ),
        name="gossip_muon",
    )(*(
        pltpu.with_memory_space_constraint(a, pltpu.HBM)
        for a in (momentum[0, 0], gradients[:, 0, 0], weights[0], outer_momentum[0])
    ))
    new_weights, new_outer = pl.pallas_call(
        write_out,
        out_shape=(
            jax.ShapeDtypeStruct((rows, cols), BF16),
            jax.ShapeDtypeStruct((block, cols), F32),
        ),
        in_specs=[vmem_spec] * 2,
        out_specs=(any_spec, any_spec),
        scratch_shapes=[dma((PIECES + 1,))],
        name="write_out",
    )(
        pltpu.with_memory_space_constraint(new_weights, pltpu.VMEM),
        pltpu.with_memory_space_constraint(new_outer, pltpu.VMEM),
    )
    return new_weights[None], new_outer[None]


def solution(mesh):
    return jax.shard_map(
        per_device,
        mesh=mesh,
        in_specs=(
            P("expert", None, None),
            P("replica", "expert", None, None),
            P(None, "replica", "expert", None, None),
            P("expert", "replica", None),
        ),
        out_specs=(P("expert", None, None), P("expert", "replica", None)),
        check_vma=False,
    )
```

```python
import functools
import math

import jax
import jax.numpy as jnp
from jax import lax
from jax.experimental import pallas as pl
from jax.experimental.pallas import tpu as pltpu
from jax.sharding import PartitionSpec as P

A, B, C = 3.4445, -4.775, 2.0315
NZ = 8
MESH = pl.DeviceIdType.MESH
F32, BF16 = jnp.float32, jnp.bfloat16

CHUNK = 32
GROUP = 128
LAG = 4

STEPS_0 = ((4, 3), (4, 3))
STEPS_1 = ((3, 4), (3, 4))
PIECES = 1
WAVES = 2
ORDER = (
    ('first', 0), ('first', 1), ('reduce', 0, 1), ('reduce', 1, 1), ('reduce', 0, 2), ('reduce', 1, 2), ('reduce', 0, 3), ('reduce', 1, 3), ('a', 0), ('a', 1), ('b', 0), ('g0', 0, 1), ('g0', 1, 1), ('b', 1), ('c', 0), ('g0', 0, 2), ('g0', 1, 2), ('c', 1), ('g1', 0, 1), ('g1', 1, 1), ('g0', 0, 3), ('g0', 1, 3), ('g1', 0, 2), ('g1', 1, 2), ('g0', 0, 4), ('g0', 1, 4), ('g1', 0, 3), ('g1', 1, 3), ('g1', 0, 4), ('g1', 1, 4),
)
X_ORDER = (4, 5, 3, 6, 2, 7, 1, 0)


def dot(a, b):
    return jnp.dot(a, b, preferred_element_type=F32)


def dot_t(a, b):
    return lax.dot_general(a, b, (((0,), (0,)), ((), ())), preferred_element_type=F32)


def kernel(
    scale, m_hbm, g_hbm, w_hbm, o_hbm, out_v, no_v,
    m_v, g_v, w_v, o_v,
    a_in, b_in, a_out, b_out, x0, gram, d0, f_v, norm, e_v, xs, xr, r0, r1, rx,
    load_sem, small_sem,
    a_recv, b_recv, ab_send, send_sem,
    xr_recv, r0_recv, r1_recv, rx_recv, g0_recv, g1_recv, gx_recv,
):
    rows, cols = m_v.shape
    half = cols // 2
    block = rows // (2 * NZ)
    part = block // WAVES
    chunks, groups, per = rows // CHUNK, rows // GROUP, GROUP // CHUNK
    me = lax.axis_index("replica")
    xl, z = me // NZ, lax.rem(me, NZ)
    over = (1 - xl) * NZ + z
    side = xl * NZ

    def at_z(offset):
        return lax.rem(z + offset + NZ, NZ)

    up, down = side + at_z(1), side + at_z(-1)
    q = lax.rem(z, 4)
    edge = jnp.logical_or(q == 0, q == 3)
    pair = side + z + 1 - 2 * lax.rem(z, 2)
    middle = side + lax.rem(jnp.where(q == 1, z + 1, z + NZ - 1), NZ)

    def send(src, dst, send_sem, recv_sem, to):
        return pltpu.make_async_remote_copy(
            src_ref=src, dst_ref=dst, send_sem=send_sem, recv_sem=recv_sem,
            device_id={"replica": to}, device_id_type=MESH,
        )

    def span(i, n):
        return pl.ds(pl.multiple_of(i * n, n), n)

    def start_load(i):
        s = span(i, GROUP)
        pltpu.make_async_copy(m_hbm.at[s], m_v.at[s], load_sem.at[i]).start()
        pltpu.make_async_copy(g_hbm.at[:, s], g_v.at[:, s], load_sem.at[i]).start()

    def wait_load(i):
        s = pl.ds(0, 2 * GROUP)
        pltpu.make_async_copy(m_hbm.at[s], m_v.at[s], load_sem.at[i]).wait()

    for i in range(groups):
        start_load(i)
    own_rows = span(me, block)
    small = (
        pltpu.make_async_copy(w_hbm.at[own_rows], w_v, small_sem.at[0]),
        pltpu.make_async_copy(o_hbm, o_v, small_sem.at[1]),
    )
    for c in small:
        c.start()

    barrier = pltpu.get_barrier_semaphore()
    for other in (up, down, over):
        pl.semaphore_signal(barrier, inc=1, device_id={"replica": other}, device_id_type=MESH)
    pl.semaphore_wait(barrier, 3)

    gram[...] = jnp.zeros_like(gram)
    norm[...] = jnp.zeros_like(norm)

    def moment(s):
        return 0.9 * m_v[s, :] + g_v[0, s, :].astype(F32)

    def send_a(i):
        s = span(i, CHUNK)
        return send(a_out.at[s], a_in.at[s], ab_send.at[0], a_recv.at[i], pair)

    def send_b(i):
        s = span(i, CHUNK)
        return send(b_out.at[s], b_in.at[s], ab_send.at[1], b_recv.at[i], middle)

    def keep(s, value):
        x0[s, :] = value.astype(BF16)
        squares = (value * value).reshape(CHUNK // 8, 8, cols)
        norm[...] += jnp.sum(squares, axis=0)

    def add_gram(j):
        x = x0[span(j, GROUP), :]
        gram[...] += dot_t(x, x)

    @pl.when(edge)
    def _():
        @pl.loop(0, groups)
        def _(j):
            wait_load(j)
            for k in range(per):
                i = j * per + k
                s = span(i, CHUNK)
                a_out[s, :] = moment(s).astype(BF16)
                send_a(i).start()

        @pl.loop(0, groups)
        def _(j):
            for k in range(per):
                i = j * per + k
                s = span(i, CHUNK)
                send_a(i).wait_recv()
                keep(s, a_in[s, :].astype(F32) + 0.225 * moment(s) + 0.5 * g_v[1, s, :].astype(F32))
            add_gram(j)

    @pl.when(jnp.logical_not(edge))
    def _():
        def second(i):
            s = span(i, CHUNK)
            send_b(i).wait_recv()
            a_out[s, :] = (b_in[s, :].astype(F32) + 0.225 * moment(s)).astype(BF16)
            send_a(i).start()

        @pl.loop(0, groups)
        def _(j):
            wait_load(j)
            for k in range(per):
                i = j * per + k
                s = span(i, CHUNK)
                send_a(i).wait_recv()
                mean = 0.5 * (a_in[s, :].astype(F32) + moment(s))
                b_out[s, :] = (0.45 * mean + 0.5 * g_v[1, s, :].astype(F32)).astype(BF16)
                send_b(i).start()
                keep(s, mean)
                if k >= LAG:
                    second(i - LAG)
                else:
                    pl.when(j > 0)(functools.partial(second, i - LAG))
            add_gram(j)

        for i in range(chunks - LAG, chunks):
            second(i)

    total = jnp.sum(jnp.sum(norm[...], axis=0, keepdims=True), axis=1, keepdims=True)
    unit = 1.0 / (jnp.sqrt(total) + 1e-7)

    g = gram[...] * (unit * unit)
    gh = g.astype(BF16)
    d = B * g + C * dot(gh, gh)
    d0[...] = d
    dh = d.astype(BF16)
    t = dot(gh, dh)
    gram[...] = (A * A) * g + (2 * A) * t + dot(t.astype(BF16), dh)

    g = gram[...]
    gh = g.astype(BF16)
    d = B * g + C * dot(gh, gh)
    dh = d.astype(BF16)
    first = d0[...]
    f_v[...] = A * (first + d) + dot(first.astype(BF16), dh)
    t = dot(gh, dh)
    gram[...] = (A * A) * g + (2 * A) * t + dot(t.astype(BF16), dh)

    g = gram[...]
    gh = g.astype(BF16)
    d = B * g + C * dot(gh, gh)
    f = f_v[...]
    e = (A * A) * d + A * f + dot(f.astype(BF16), d.astype(BF16))
    factor = unit * scale
    e_v[...] = (e * factor).astype(BF16)
    lead = factor * (A * A * A)

    def send_xr(v, k):
        zz = at_z(k)
        src = xs.at[0, v, (1 - xl) * NZ + zz]
        return send(src, xr.at[v, zz], send_sem.at[0], xr_recv.at[v, k], over)

    def slot(steps, way, t):
        return (0 if way > 0 else steps[0]) + t - 1

    def steps_of(steps, way):
        return steps[0] if way > 0 else steps[1]

    def towards(way):
        return up if way > 0 else down

    def x_of(jj):
        return 1 - xl if jj == 0 else xl

    def send_r0(v, way, t, src):
        i = slot(STEPS_0[v], way, t)
        return send(src, r0.at[v, i], send_sem.at[0], r0_recv.at[v, i], towards(way))

    def send_r1(v, jj, way, t, src):
        i = slot(STEPS_1[v], way, t)
        return send(src, r1.at[v, jj, i], send_sem.at[0], r1_recv.at[v, i], towards(way))

    def wait_r1(v, i):
        r = pl.ds(0, part)
        send(a_out.at[r], a_in.at[r], send_sem.at[0], r1_recv.at[v, i], pair).wait_recv()

    def offset(way, n, t):
        return way * (n + 1 - t)

    sent = [0, 0]

    def go(c, phase=0):
        sent[phase] += part // 2
        c.start()

    e = e_v[...]
    for k in X_ORDER:
        zz = at_z(k)
        x = jnp.concatenate([x0[span(zz, block), :], x0[span(NZ + zz, block), :]], axis=0)
        y = (lead * x.astype(F32) + dot(x, e)).astype(BF16)
        for v in range(WAVES):
            for h in range(2):
                c = slice(h * half, (h + 1) * half)
                xs[h, v, zz] = y[v * part : (v + 1) * part, c]
                xs[h, v, NZ + zz] = y[block + v * part : block + (v + 1) * part, c]
        for v in range(WAVES):
            go(send_xr(v, k))
            for way in (1, -1):
                n = steps_of(STEPS_1[v], way)
                if (way * n) % NZ == k:
                    for jj in range(2):
                        go(send_r1(v, jj, way, 1, xs.at[1, v, x_of(jj) * NZ + zz]))

    def own_0(v, k):
        send_xr(v, k % NZ).wait_recv()
        zz = at_z(k)
        return zz, xs[0, v, side + zz].astype(F32) + xr[v, zz].astype(F32)

    def first_0(v):
        for way in (1, -1):
            zz, own = own_0(v, offset(way, steps_of(STEPS_0[v], way), 1))
            xr[v, zz] = own.astype(BF16)
            go(send_r0(v, way, 1, xr.at[v, zz]))

    def forward_0(v, way, t):
        n = steps_of(STEPS_0[v], way)
        i = slot(STEPS_0[v], way, t)
        send_r0(v, way, t, r0.at[v, i]).wait_recv()
        _, own = own_0(v, offset(way, n, t + 1))
        r0[v, i] = (r0[v, i].astype(F32) + own).astype(BF16)
        go(send_r0(v, way, t + 1, r0.at[v, i]))

    def forward_1(v, jj, way, t):
        n = steps_of(STEPS_1[v], way)
        i = slot(STEPS_1[v], way, t)
        if jj == 0:
            wait_r1(v, i)
        own = xs[1, v, x_of(jj) * NZ + at_z(offset(way, n, t + 1))]
        r1[v, jj, i] = (r1[v, jj, i].astype(F32) + own.astype(F32)).astype(BF16)
        go(send_r1(v, jj, way, t + 1, r1.at[v, jj, i]))

    def reduce_step(v, t):
        for jj in range(2):
            for way in (1, -1):
                if t < steps_of(STEPS_1[v], way):
                    forward_1(v, jj, way, t)
        for way in (1, -1):
            if t < steps_of(STEPS_0[v], way):
                forward_0(v, way, t)

    def last_1(v, jj):
        out = xs[1, v, x_of(jj) * NZ + z].astype(F32)
        for way in (1, -1):
            n = steps_of(STEPS_1[v], way)
            i = slot(STEPS_1[v], way, n)
            if jj == 0:
                wait_r1(v, i)
            out += r1[v, jj, i].astype(F32)
        return out

    def last_0(v):
        _, out = own_0(v, 0)
        for way in (1, -1):
            n = steps_of(STEPS_0[v], way)
            i = slot(STEPS_0[v], way, n)
            send_r0(v, way, n, r0.at[v, i]).wait_recv()
            out += r0[v, i].astype(F32)
        return out

    def cross(v):
        src = xs.at[1, v, (1 - xl) * NZ + z]
        return send(src, rx.at[v], send_sem.at[0], rx_recv.at[v], over)

    def rows_of(v, b):
        return pl.ds(pl.multiple_of(b * block + v * part, part), part)

    def piece(v, b, h):
        return out_v.at[rows_of(v, b), pl.ds(h * half, half)]

    def outer(v, h, delta):
        r, c = slice(v * part, (v + 1) * part), slice(h * half, (h + 1) * half)
        fresh = 0.9 * o_v[r, c] + delta
        no_v[r, c] = fresh
        out_v[rows_of(v, me), c] = (w_v[r, c].astype(F32) - fresh).astype(BF16)

    def send_g0(v, way, t, p):
        i = slot(STEPS_0[v], way, t)
        return send(p, p, send_sem.at[1], g0_recv.at[v, i], towards(way))

    def send_g1(v, jj, way, t, p):
        i = slot(STEPS_1[v], way, t)
        return send(p, p, send_sem.at[1], g1_recv.at[v, jj, i], towards(way))

    def send_gx(v, k, p):
        return send(p, p, send_sem.at[1], gx_recv.at[v, k // NZ], over)

    def gather_0(v, t):
        for way in (1, -1):
            n = steps_of(STEPS_0[v], way)
            if t <= n:
                k = (-way * t) % NZ
                p = piece(v, side + at_z(k), 0)
                send_g0(v, way, t, p).wait_recv()
                if t < n:
                    go(send_g0(v, way, t + 1, p), 1)
                go(send_gx(v, k, p), 1)

    def gather_1(v, t):
        for jj in (1, 0):
            for way in (1, -1):
                n = steps_of(STEPS_1[v], way)
                if t <= n:
                    p = piece(v, x_of(jj) * NZ + at_z(-way * t), 1)
                    send_g1(v, jj, way, t, p).wait_recv()
                    if t < n:
                        go(send_g1(v, jj, way, t + 1, p), 1)

    def end_a(v):
        xs[1, v, (1 - xl) * NZ + z] = last_1(v, 0).astype(BF16)
        go(cross(v))
        outer(v, 0, last_0(v))
        p = piece(v, me, 0)
        for way in (1, -1):
            go(send_g0(v, way, 1, p), 1)
        go(send_gx(v, 0, p), 1)

    def end_b(v):
        total_1 = last_1(v, 1)
        cross(v).wait_recv()
        outer(v, 1, total_1 + rx[v].astype(F32))
        p = piece(v, me, 1)
        go(send_gx(v, NZ, p), 1)
        for way in (1, -1):
            go(send_g1(v, 1, way, 1, p), 1)

    def end_c(v):
        p = piece(v, over, 1)
        send_gx(v, NZ, p).wait_recv()
        for way in (1, -1):
            go(send_g1(v, 0, way, 1, p), 1)

    steps = dict(
        first=first_0, reduce=reduce_step, a=end_a, b=end_b, c=end_c, g0=gather_0, g1=gather_1
    )
    for c in small:
        c.wait()
    for step, *args in ORDER:
        steps[step](*args)
    for v in range(WAVES):
        r = pl.ds(0, NZ * part // 2)
        send(a_out.at[r], a_in.at[r], send_sem.at[1], gx_recv.at[v, 0], over).wait_recv()

    for phase in range(2):
        r = pl.ds(0, sent[phase])
        send(a_out.at[r], a_in.at[r], send_sem.at[phase], a_recv.at[0], pair).wait_send()
    send(a_out, a_in, ab_send.at[0], a_recv.at[0], pair).wait_send()

    @pl.when(jnp.logical_not(edge))
    def _():
        send(b_out, b_in, ab_send.at[1], b_recv.at[0], middle).wait_send()


def write_out(w_v, o_v, w_hbm, o_hbm, sem):
    n = w_v.shape[0] // PIECES
    copies = [pltpu.make_async_copy(o_v, o_hbm, sem.at[PIECES])]
    for i in range(PIECES):
        s = pl.ds(i * n, n)
        copies.append(pltpu.make_async_copy(w_v.at[s], w_hbm.at[s], sem.at[i]))
    for c in copies:
        c.start()
    for c in copies:
        c.wait()


def per_device(weights, momentum, gradients, outer_momentum):
    rows, cols = weights.shape[1:]
    half, block = cols // 2, rows // (2 * NZ)
    part = block // WAVES
    chunks, groups = rows // CHUNK, rows // GROUP
    scale = 2 * 0.5 * 0.2 * math.sqrt(rows) / (2 * NZ)
    hbm_spec = pl.BlockSpec(memory_space=pltpu.HBM)
    any_spec = pl.BlockSpec(memory_space=pl.ANY)
    vmem_spec = pl.BlockSpec(memory_space=pltpu.VMEM)
    dma = pltpu.SemaphoreType.DMA
    new_weights, new_outer = pl.pallas_call(
        functools.partial(kernel, scale),
        out_shape=(pltpu.VMEM((rows, cols), BF16), pltpu.VMEM((block, cols), F32)),
        in_specs=[hbm_spec] * 4,
        out_specs=(vmem_spec, vmem_spec),
        scratch_shapes=[
            pltpu.VMEM((rows, cols), F32),
            pltpu.VMEM((2, rows, cols), BF16),
            pltpu.VMEM((block, cols), BF16),
            pltpu.VMEM((block, cols), F32),
            pltpu.VMEM((rows, cols), BF16),
            pltpu.VMEM((rows, cols), BF16),
            pltpu.VMEM((rows, cols), BF16),
            pltpu.VMEM((rows, cols), BF16),
            pltpu.VMEM((rows, cols), BF16),
            pltpu.VMEM((cols, cols), F32),
            pltpu.VMEM((cols, cols), F32),
            pltpu.VMEM((cols, cols), F32),
            pltpu.VMEM((8, cols), F32),
            pltpu.VMEM((cols, cols), BF16),
            pltpu.VMEM((2, WAVES, 2 * NZ, part, half), BF16),
            pltpu.VMEM((WAVES, NZ, part, half), BF16),
            pltpu.VMEM((WAVES, NZ - 1, part, half), BF16),
            pltpu.VMEM((WAVES, 2, NZ - 1, part, half), BF16),
            pltpu.VMEM((WAVES, part, half), BF16),
            dma((groups,)),
            dma((2,)),
            dma((chunks,)), dma((chunks,)), dma((2,)),
            dma((2,)),
            dma((WAVES, NZ)),
            dma((WAVES, NZ - 1)),
            dma((WAVES, NZ - 1)),
            dma((WAVES,)),
            dma((WAVES, NZ - 1)),
            dma((WAVES, 2, NZ - 1)),
            dma((WAVES, 2)),
        ],
        compiler_params=pltpu.CompilerParams(
            collective_id=0, has_side_effects=True, vmem_limit_bytes=48 * 1024 * 1024
        ),
        name="gossip_muon",
    )(*(
        pltpu.with_memory_space_constraint(a, pltpu.HBM)
        for a in (momentum[0, 0], gradients[:, 0, 0], weights[0], outer_momentum[0])
    ))
    new_weights, new_outer = pl.pallas_call(
        write_out,
        out_shape=(
            jax.ShapeDtypeStruct((rows, cols), BF16),
            jax.ShapeDtypeStruct((block, cols), F32),
        ),
        in_specs=[vmem_spec] * 2,
        out_specs=(any_spec, any_spec),
        scratch_shapes=[dma((PIECES + 1,))],
        name="write_out",
    )(
        pltpu.with_memory_space_constraint(new_weights, pltpu.VMEM),
        pltpu.with_memory_space_constraint(new_outer, pltpu.VMEM),
    )
    return new_weights[None], new_outer[None]


def solution(mesh):
    return jax.shard_map(
        per_device,
        mesh=mesh,
        in_specs=(
            P("expert", None, None),
            P("replica", "expert", None, None),
            P(None, "replica", "expert", None, None),
            P("expert", "replica", None),
        ),
        out_specs=(P("expert", None, None), P("expert", "replica", None)),
        check_vma=False,
    )
```
